32 devices in a mesh: groups: 2 (over y), users: 4 (over z), routers: 2 (over x), heads: 2 (over core).
Axes of the slice: x: 2, y: 2, z: 4, core: 2. Of those that a mesh axis runs over, the one named last changes fastest.
Arguments:
- items: bfloat16 [64, 64, 1024], P(('groups', 'users', 'routers')), parts along dimension 0, may hold values from -6 to 6
- block_owner: int32 [64, 1], P(('groups', 'users', 'routers')), parts along dimension 0, may hold values from 0 to 3; in each aligned block of 4 rows (0 to 3, 4 to 7, ...) at most 2 rows name the same one
- block_user: int32 [64], P(('groups', 'users', 'routers')), parts along dimension 0, may hold values from 0 to 1
- block_fill: int32 [64], P(('groups', 'users', 'routers')), parts along dimension 0, may hold values from 1 to 64
- prefix_keys: bfloat16 [16, 256, 1024], P(('groups', 'users'), None, 'heads'), parts along dimension 0, may hold values from -6 to 6
- prefix_values: bfloat16 [16, 256, 1024], P(('groups', 'users'), None, 'heads'), parts along dimension 0, may hold values from -6 to 6
- w_in: bfloat16 [4, 1024, 1024], P(None, 'routers', 'heads'), may hold values from -0.1875 to 0.1875
- attn_gain: bfloat16 [1024], P('heads'), may hold values from 0.25 to 1.75
- w_o: bfloat16 [1024, 1024], P('heads', 'routers'), may hold values from -0.1875 to 0.1875
- mlp_gain: bfloat16 [1024], replicated, may hold values from 0.25 to 1.75
- w_one: bfloat16 [1024, 256], replicated, may hold values from -0.1875 to 0.1875
- w_two: bfloat16 [256], replicated, may hold values from -0.375 to 0.375
Outputs:
- scores: float32 [64, 64], P(('groups', 'users', 'routers')), parts along dimension 0
The draws below stay inside these ranges and needn't reach their ends.
There are 2 independent parts, one for each index of `groups`. The reference program is written for one: setup_inputs(seed, part) draws one part's arguments, and reference() takes and returns one part's arrays. A program takes and returns all parts, laid end to end along the dimension named above; an argument that names none is the same for every part. Nothing has to cross between parts.
Inputs may be any that keep to these rules, and one draw needn't show every extreme that they name: `block_owner`: within the rows of one device (aligned blocks of 4 blocks), no owner is named by more than 2 rows, and in every draw some owner is named by exactly 2 rows of some device.
All inputs are finite; a program needn't handle non-finite values.
Results may differ from the reference program's by a relative error of at most 0.005.
Values may be sent and summed in bfloat16 or wider, within the bound.
A program may use at most 64 MiB of HBM per device.

```python
import math
import jax
import jax.numpy as jnp
import numpy as np
from jax import lax

D = 1024
HEADS = 8
HEAD_DIM = 128
HID = 256
BLOCK = 64
CAP = 2
LPRE = 256
USR_DEV = 2
BLK_DEV = 4
HD = 1024
USERS = 8
NBLK = 32
N_USERS = 4


def touch_ends(drawn, own_key, smallest, largest):
    index_at = [jax.random.randint(jax.random.fold_in(own_key, axis), (), 0, length) for axis, length in enumerate(drawn.shape)]
    widest = drawn.shape.index(max(drawn.shape))
    beside = index_at[:widest] + [(index_at[widest] + 1) % drawn.shape[widest]] + index_at[widest + 1:]
    return drawn.at[tuple(index_at)].set(smallest).at[tuple(beside)].set(largest)


def block_scale(rng, dims, split, least, top_value):
    factor_of = 1.0
    for position, shards_of in split:
        draws = jax.random.uniform(jax.random.fold_in(jax.random.fold_in(rng, 6), position), (shards_of,), jnp.float32, least / len(split), top_value / len(split))
        factor_of = factor_of * jnp.repeat(jnp.exp(draws), dims[position] // shards_of).reshape((-1,) + (1,) * (len(dims) - 1 - position))
    return factor_of


def assign_block(rng, own, number, rows, amount, top, limit, skew):
    ranking = jax.random.permutation(rng, amount)
    crowded, ordinary = portions_of(amount, rows * top, limit, skew, True), portions_of(amount, rows * top, limit, skew, False)
    places = jnp.arange(amount)

    def named(tallies, offset_by):
        used = int((tallies > 0).sum())
        fixed = max(1, used // 4)
        passed = fixed + (places - fixed + offset_by * (used - fixed)) % max(1, amount - fixed)
        return jnp.zeros((amount,), jnp.int32).at[ranking[jnp.where(places < fixed, places, passed)]].set(jnp.asarray(tallies, jnp.int32))

    tallies = jnp.where(number % 4 == 0, named(crowded, number // 4), named(ordinary, number - number // 4 - 1))
    mixed = jax.random.permutation(jax.random.fold_in(own, 3), amount)
    source_of, sink = mixed[0:amount // 2 * 2:2], mixed[1:amount // 2 * 2:2]
    slack = jnp.minimum(tallies[source_of] - 1, limit - tallies[sink]) // 2
    slack = jnp.where((source_of == ranking[0]) | (sink == ranking[0]) | (tallies[sink] == 0), 0, jnp.maximum(slack, 0))
    passed = jax.random.randint(jax.random.fold_in(own, 4), (amount // 2,), 0, 1 << 20) % (slack + 1)
    tallies = tallies.at[source_of].add(-passed).at[sink].add(passed)
    items = jnp.searchsorted(jnp.cumsum(tallies), jnp.arange(rows * top), side="right").astype(jnp.int32)
    listing = items.reshape(top, rows).T
    listing = listing[jax.random.permutation(jax.random.fold_in(own, 1), rows)]
    offset_by = jax.random.randint(jax.random.fold_in(own, 2), (rows, 1), 0, top)
    return jnp.take_along_axis(listing, (jnp.arange(top)[None, :] + offset_by) % top, axis=1)


def portions_of(number_of, total, reach, lean, full):
    portions = [(1 << 20) // math.isqrt(rank ** lean) + 1 for rank in range(1, number_of + 1)]
    largest = reach if full else min(reach, max(-(-total // number_of), total * portions[0] // sum(portions)))
    least = 1 if total - largest >= number_of - 1 else 0
    counts, rest = [largest] + [least] * (number_of - 1), total - largest - least * (number_of - 1)
    while rest > 0:
        movable = [i for i in range(1, number_of) if counts[i] < largest] or [i for i in range(1, number_of) if counts[i] < reach]
        pool, remaining = sum([portions[i] for i in movable]), rest
        for i in movable:
            addition = min(reach - counts[i], max(1, remaining * portions[i] // pool), rest)
            counts[i] = counts[i] + addition
            rest = rest - addition
    return np.array(counts)


def gaussian(rng, dims, scale, most, shards=(), held_as=jnp.bfloat16):
    gain = block_scale(rng, dims, shards, -0.22, 0.18) if shards else 1.0
    values = jax.random.normal(rng, dims, jnp.float32) * scale * gain
    return jnp.minimum(jnp.maximum(values, -most), most).astype(held_as)


def setup_inputs(seed: int = 0, part: int = 0) -> dict:
    seeds = jax.random.split(jax.random.key(seed), 13)
    part_splits = jax.random.split(jax.random.fold_in(seeds[12], part), 13)
    items = gaussian(part_splits[0], (NBLK, BLOCK, D), 1.0, 6.0, ((0, 8),))
    block_owner_keys = jax.random.split(jax.random.fold_in(part_splits[1], 1), NBLK // BLK_DEV)
    block_owner_turns = jax.random.permutation(jax.random.fold_in(part_splits[1], 3), NBLK // BLK_DEV)
    block_owner = jax.vmap(lambda own, number: assign_block(jax.random.fold_in(part_splits[1], 2), own, number, BLK_DEV, N_USERS, 1, CAP, 2))(block_owner_keys, block_owner_turns).reshape((NBLK, 1))
    block_user = touch_ends(jax.random.randint(part_splits[2], (NBLK,), 0, USR_DEV), jax.random.fold_in(part_splits[2], 1), 0, USR_DEV - 1).astype(jnp.int32)
    block_fill = touch_ends(jax.random.randint(part_splits[3], (NBLK,), 1, BLOCK + 1), jax.random.fold_in(part_splits[3], 1), 1, BLOCK).astype(jnp.int32)
    prefix_keys = gaussian(part_splits[4], (USERS, LPRE, HD), 1.0, 6.0, ((0, 4), (2, 2)))
    prefix_values = gaussian(part_splits[5], (USERS, LPRE, HD), 1.0, 6.0, ((0, 4), (2, 2)))
    w_in = gaussian(seeds[6], (4, D, HD), D ** -0.5, 0.1875, ((1, 2), (2, 2)))
    attn_gain = jnp.clip(1.0 + 0.15 * jax.random.normal(seeds[7], (HD,), jnp.float32), 0.25, 1.75).astype(jnp.bfloat16)
    w_o = gaussian(seeds[8], (HD, D), HD ** -0.5, 0.1875, ((0, 2), (1, 2)))
    mlp_gain = jnp.clip(1.0 + 0.15 * jax.random.normal(seeds[9], (D,), jnp.float32), 0.25, 1.75).astype(jnp.bfloat16)
    w_one = gaussian(seeds[10], (D, HID), D ** -0.5, 0.1875)
    w_two = gaussian(seeds[11], (HID,), HID ** -0.5, 0.375)
    return dict(items=items, block_owner=block_owner, block_user=block_user, block_fill=block_fill, prefix_keys=prefix_keys, prefix_values=prefix_values, w_in=w_in, attn_gain=attn_gain, w_o=w_o, mlp_gain=mlp_gain, w_one=w_one, w_two=w_two)


def score_block(block_items, owner_index, user_index, fill_count, prefix_keys, prefix_values, wide_in, attn_gain, w_o, mlp_gain, w_one, w_two):
    score_scale = HEAD_DIM ** (-0.5)
    cache_slot = (owner_index * USR_DEV + user_index).astype(jnp.int32)
    user_keys = lax.dynamic_index_in_dim(prefix_keys, cache_slot, 0, keepdims=False)
    user_values = lax.dynamic_index_in_dim(prefix_values, cache_slot, 0, keepdims=False)
    projected = jax.nn.silu(jnp.einsum('rk,pkc->prc', block_items.astype(jnp.float32), wide_in))
    queries = projected[0].astype(jnp.bfloat16)
    query_heads = queries.astype(jnp.float32).reshape(BLOCK, HEADS, HEAD_DIM)
    key_heads = user_keys.astype(jnp.float32).reshape(LPRE, HEADS, HEAD_DIM)
    value_heads = user_values.astype(jnp.float32).reshape(LPRE, HEADS, HEAD_DIM)
    raw_scores = jnp.einsum('qhd,khd->hqk', query_heads, key_heads) * score_scale
    weights = jax.nn.silu(raw_scores).astype(jnp.bfloat16)
    prefix_part = jnp.einsum('hqk,khd->qhd', weights.astype(jnp.float32), value_heads).astype(jnp.bfloat16)
    self_keys = projected[1].reshape(BLOCK, HEADS, HEAD_DIM)
    self_values = projected[2].reshape(BLOCK, HEADS, HEAD_DIM)
    gates = projected[3]
    own_term = jax.nn.silu(lax.optimization_barrier(jnp.sum(query_heads * self_keys, axis=-1)) * score_scale)[..., None] * self_values
    attended = (prefix_part.astype(jnp.float32) + own_term).reshape(BLOCK, HD)
    row_mean = lax.optimization_barrier(jnp.sum(attended, axis=1)) / HD
    row_var = lax.optimization_barrier(jnp.sum(attended * attended, axis=1)) / HD - row_mean * row_mean
    gated = ((attended - row_mean[:, None]) * lax.rsqrt(row_var + 1e-05)[:, None] * attn_gain.astype(jnp.float32) * gates).astype(jnp.bfloat16)
    residual = block_items.astype(jnp.float32) + jnp.dot(gated, w_o, preferred_element_type=jnp.float32)
    row_scale = lax.rsqrt(lax.optimization_barrier(jnp.sum(residual * residual, axis=1)) / D + 1e-05)
    normed = (residual * row_scale[:, None] * mlp_gain.astype(jnp.float32)).astype(jnp.bfloat16)
    hidden = jax.nn.silu(jnp.dot(normed, w_one, preferred_element_type=jnp.float32)).astype(jnp.bfloat16)
    block_scores = jnp.dot(hidden, w_two, preferred_element_type=jnp.float32)
    is_valid = jnp.arange(BLOCK, dtype=jnp.int32) < fill_count
    return jnp.where(is_valid, block_scores, jnp.zeros_like(block_scores))

def reference(items, block_owner, block_user, block_fill, prefix_keys, prefix_values, w_in, attn_gain, w_o, mlp_gain, w_one, w_two):
    wide_in = w_in.astype(jnp.float32)

    def one_block(packed):
        block_items, owner_index, user_index, fill_count = packed
        return score_block(block_items, owner_index, user_index, fill_count, prefix_keys, prefix_values, wide_in, attn_gain, w_o, mlp_gain, w_one, w_two)
    return lax.map(one_block, (items, block_owner[:, 0], block_user, block_fill))
```

```python
import functools

import jax
import jax.numpy as jnp
from jax import lax
from jax.experimental import pallas as pl
from jax.experimental.pallas import tpu as pltpu
from jax.sharding import PartitionSpec as P

HEAD_DIM = 128
CAP = 2
EPSILON = 1e-05
SUB = 2
F32 = jnp.float32
BF16 = jnp.bfloat16
MESH = pl.DeviceIdType.MESH


def silu(v):
    return 0.5 * v * (1.0 + jnp.tanh(0.5 * v))


def scorer(
    sizes,
    items_ref,
    owner_ref,
    user_ref,
    fill_ref,
    keys_ref,
    values_ref,
    w_in_ref,
    attn_gain_ref,
    w_o_ref,
    mlp_gain_ref,
    w_one_ref,
    w_two_ref,
    out_ref,
    items_v,
    out_slots,
    x_all,
    mask_out,
    mask_all,
    keys_v,
    values_v,
    w_all,
    wo_all,
    w_one_v,
    q_v,
    sk_v,
    sv_v,
    gates_v,
    att_v,
    gated_v,
    stat_out,
    stat_in,
    part_out,
    part_own,
    part_in,
    sc_out,
    ret,
    local_sem,
    z_send,
    z_recv,
    m_send,
    m_recv,
    rel_send,
    rel_recv,
    x_send,
    x_recv,
    y_send,
    y_recv,
    st_sem,
    po_send,
    po_recv,
    sc_send,
    sc_recv,
):
    groups, users, routers, heads = sizes
    g = lax.axis_index("groups")
    me = lax.axis_index("users")
    r = lax.axis_index("routers")
    h = lax.axis_index("heads")
    mate = 1 - h
    blocks, width, model = items_v.shape
    slots = x_all.shape[0]
    half_width = q_v.shape[1]
    heads_here = half_width // HEAD_DIM
    hd_all = half_width * heads
    rows = slots * width
    depth = w_all.shape[2]
    out_cols = wo_all.shape[2]
    wh = width // heads
    scale = HEAD_DIM ** (-0.5)
    positions = keys_v.shape[0] * keys_v.shape[1]
    per_user = keys_v.shape[1]

    c_items = pltpu.make_async_copy(items_ref, items_v, local_sem.at[0])
    c_items.start()

    barrier = pltpu.get_barrier_semaphore()
    count = 0
    for j in range(1, routers):
        pl.semaphore_signal(
            barrier, inc=1, device_id={"routers": lax.rem(r + j, routers)}, device_id_type=MESH
        )
        count += 1
    for i in range(1, groups):
        pl.semaphore_signal(
            barrier, inc=1, device_id={"groups": lax.rem(g + i, groups)}, device_id_type=MESH
        )
        count += 1
    pl.semaphore_signal(barrier, inc=1, device_id={"heads": mate}, device_id_type=MESH)
    count += 1
    for k in range(1, users):
        for e in range(heads):
            pl.semaphore_signal(
                barrier,
                inc=1,
                device_id={"users": lax.rem(me + k, users), "heads": e},
                device_id_type=MESH,
            )
            count += 1
    c_keys = pltpu.make_async_copy(keys_ref, keys_v, local_sem.at[1])
    c_values = pltpu.make_async_copy(values_ref, values_v, local_sem.at[2])
    c_win = pltpu.make_async_copy(w_in_ref, w_all.at[:, r], local_sem.at[3])
    c_wo = pltpu.make_async_copy(w_o_ref, wo_all.at[r], local_sem.at[4])
    c_one = pltpu.make_async_copy(w_one_ref, w_one_v, local_sem.at[5])
    pl.semaphore_wait(barrier, count)

    pieces = [(p, s) for p in range(5) for s in range(SUB)]

    def in_rows(owner_group, s):
        share = depth // groups // SUB
        return pl.ds(pl.multiple_of((owner_group * SUB + s) * share, share), share)

    def out_rows(owner_group, s):
        share = half_width // groups // SUB
        return pl.ds(pl.multiple_of((owner_group * SUB + s) * share, share), share)

    def weight_slot(owner_router, owner_group, p, s):
        if p < 4:
            return w_all.at[p, owner_router, in_rows(owner_group, s), :]
        return wo_all.at[owner_router, out_rows(owner_group, s), :]

    def x_copy(j, t, source_router):
        p, s = pieces[t]
        if p < 4:
            src = w_in_ref.at[p, in_rows(g, s), :]
        else:
            src = w_o_ref.at[out_rows(g, s), :]
        return pltpu.make_async_remote_copy(
            src_ref=src,
            dst_ref=weight_slot(source_router, g, p, s),
            send_sem=x_send.at[j, t],
            recv_sem=x_recv.at[j, t],
            device_id={"routers": lax.rem(r + j, routers)},
            device_id_type=MESH,
        )

    def y_copy(i, j, t, owner_group):
        p, s = pieces[t]
        spot = weight_slot(lax.rem(r - j + routers, routers), owner_group, p, s)
        return pltpu.make_async_remote_copy(
            src_ref=spot,
            dst_ref=spot,
            send_sem=y_send.at[i, j, t],
            recv_sem=y_recv.at[i, j, t],
            device_id={"groups": lax.rem(g + i, groups)},
            device_id_type=MESH,
        )

    for t in range(len(pieces)):
        for j in range(1, routers):
            x_copy(j, t, r).start()
    for c in (c_win, c_keys, c_values, c_wo, c_one):
        c.start()

    owners = [owner_ref[b, 0] for b in range(blocks)]
    ranks = []
    for b in range(blocks):
        rank = jnp.int32(0)
        for a in range(b):
            rank = rank + jnp.where(owners[a] == owners[b], 1, 0)
        ranks.append(rank)

    def slot_source(dest, cap):
        index, user = jnp.int32(0), jnp.int32(-1)
        for b in range(blocks):
            hit = (owners[b] == dest) & (ranks[b] == cap)
            index = jnp.where(hit, b, index)
            user = jnp.where(hit, user_ref[b], user)
        return index, user

    lane_user = lax.broadcasted_iota(jnp.int32, (1, positions), 1) // per_user
    mask_copies, item_copies = {}, {}

    def z_copy(k, source):
        return pltpu.make_async_remote_copy(
            src_ref=out_slots.at[k],
            dst_ref=x_all.at[pl.ds(source * CAP, CAP), pl.ds(pl.multiple_of(h * wh, wh), wh), :],
            send_sem=z_send.at[k],
            recv_sem=z_recv.at[k],
            device_id={"users": lax.rem(me + k, users)},
            device_id_type=MESH,
        )

    def m_copy(k, source):
        return pltpu.make_async_remote_copy(
            src_ref=mask_out.at[k],
            dst_ref=mask_all.at[source],
            send_sem=m_send.at[k],
            recv_sem=m_recv.at[k],
            device_id={"users": lax.rem(me + k, users)},
            device_id_type=MESH,
        )

    def relay_copy(k, part):
        source = lax.rem(me - k + users, users)
        spot = x_all.at[pl.ds(source * CAP, CAP), pl.ds(pl.multiple_of(part * wh, wh), wh), :]
        return pltpu.make_async_remote_copy(
            src_ref=spot,
            dst_ref=spot,
            send_sem=rel_send.at[k],
            recv_sem=rel_recv.at[k],
            device_id={"heads": mate},
            device_id_type=MESH,
        )

    c_items.wait()
    for k in list(range(1, users)) + [0]:
        dest = lax.rem(me + k, users)
        for cap in range(CAP):
            index, user = slot_source(dest, cap)
            line = jnp.where(lane_user == user, 1.0, 0.0).astype(F32)
            if k == 0:
                x_all[me * CAP + cap] = items_v[index]
                mask_all[me, cap : cap + 1, :] = line
            else:
                out_slots[k, cap] = items_v[index, pl.ds(pl.multiple_of(h * wh, wh), wh), :]
                mask_out[k, cap : cap + 1, :] = line
        if k:
            z_copy(k, me).start()
            m_copy(k, me).start()

    def forward(t):
        for j in range(1, routers):
            x_copy(j, t, lax.rem(r - j + routers, routers)).wait_recv()
            for i in range(1, groups):
                y_copy(i, j, t, g).start()

    def landed(t):
        for j in range(1, routers):
            for i in range(1, groups):
                y_copy(i, j, t, lax.rem(g - i + groups, groups)).wait_recv()

    forward(0)
    forward(1)
    for k in range(1, users):
        z_copy(k, lax.rem(me - k + users, users)).wait_recv()
        relay_copy(k, h).start()
    forward(2)
    for k in range(1, users):
        m_copy(k, lax.rem(me - k + users, users)).wait_recv()
        relay_copy(k, mate).wait_recv()
    c_win.wait()

    tile = 4 * width
    tile_slots = 4
    tiles = rows // tile

    def x_tile(i):
        return x_all[pl.ds(i * tile_slots, tile_slots)].reshape(tile, model)

    def project(p, target):
        @pl.loop(0, tiles)
        def _(i):
            x = x_tile(i)
            total = jnp.zeros((tile, half_width), F32)
            for a in range(routers):
                total = total + jnp.dot(
                    x[:, a * depth : (a + 1) * depth],
                    w_all[p, a],
                    preferred_element_type=F32,
                )
            target[pl.ds(pl.multiple_of(i * tile, tile), tile), :] = silu(total).astype(target.dtype)

    landed(0)
    landed(1)
    project(0, q_v)
    forward(3)
    c_keys.wait()
    c_values.wait()

    @pl.loop(0, tiles)
    def _(i):
        span = pl.ds(pl.multiple_of(i * tile, tile), tile)
        for e in range(heads_here):
            cols = slice(e * HEAD_DIM, (e + 1) * HEAD_DIM)
            raw = lax.dot_general(
                q_v[span, cols],
                keys_v[:, :, cols].reshape(positions, HEAD_DIM),
                (((1,), (1,)), ((), ())),
                preferred_element_type=F32,
            )
            weights = silu(raw * scale)
            parts = []
            for s in range(tile_slots):
                line = mask_all[i * (tile_slots // CAP) + s // CAP, s % CAP : s % CAP + 1, :]
                parts.append(weights[s * width : (s + 1) * width] * line)
            weights = jnp.concatenate(parts, axis=0).astype(BF16)
            att_v[span, cols] = (
                jnp.dot(
                    weights,
                    values_v[:, :, cols].reshape(positions, HEAD_DIM),
                    preferred_element_type=F32,
                )
                .astype(BF16)
                .astype(F32)
            )

    forward(4)
    landed(2)
    landed(3)
    project(1, sk_v)
    forward(5)
    forward(6)
    landed(4)
    landed(5)
    project(2, sv_v)
    forward(7)

    lane = lax.broadcasted_iota(jnp.int32, (tile, 128), 1)

    @pl.loop(0, tiles)
    def _(i):
        span = pl.ds(pl.multiple_of(i * tile, tile), tile)
        total = jnp.zeros((tile, 1), F32)
        square = jnp.zeros((tile, 1), F32)
        for e in range(heads_here):
            cols = slice(e * HEAD_DIM, (e + 1) * HEAD_DIM)
            own = jnp.sum(q_v[span, cols].astype(F32) * sk_v[span, cols], axis=1, keepdims=True)
            att = att_v[span, cols] + silu(own * scale) * sv_v[span, cols]
            att_v[span, cols] = att
            total = total + jnp.sum(att, axis=1, keepdims=True)
            square = square + jnp.sum(att * att, axis=1, keepdims=True)
        stat_out[span, :] = jnp.where(lane == 0, total, square)

    stat_copy = pltpu.make_async_remote_copy(
        src_ref=stat_out,
        dst_ref=stat_in,
        send_sem=st_sem.at[0],
        recv_sem=st_sem.at[1],
        device_id={"heads": mate},
        device_id_type=MESH,
    )
    stat_copy.start()
    forward(8)
    landed(6)
    landed(7)
    project(3, gates_v)
    forward(9)
    stat_copy.wait_recv()

    @pl.loop(0, tiles)
    def _(i):
        span = pl.ds(pl.multiple_of(i * tile, tile), tile)
        both = stat_out[span, :] + stat_in[span, :]
        mean = both[:, 0:1] / hd_all
        var = both[:, 1:2] / hd_all - mean * mean
        gated_v[span, :] = (
            (att_v[span, :] - mean)
            * lax.rsqrt(var + EPSILON)
            * attn_gain_ref[...].astype(F32)
            * gates_v[span, :]
        ).astype(BF16)

    half = rows // heads
    half_tiles = half // tile
    c_wo.wait()

    def part_copy(j):
        return pltpu.make_async_remote_copy(
            src_ref=part_out.at[j],
            dst_ref=part_in.at[j],
            send_sem=po_send.at[j],
            recv_sem=po_recv.at[j],
            device_id={"heads": mate},
            device_id_type=MESH,
        )

    def out_project(j, row_half, target):
        a = lax.rem(r - j + routers, routers)

        @pl.loop(0, half_tiles)
        def _(i):
            src = pl.ds(pl.multiple_of(row_half * half + i * tile, tile), tile)
            target[j, pl.ds(pl.multiple_of(i * tile, tile), tile), :] = jnp.dot(
                gated_v[src, :], wo_all[a], preferred_element_type=F32
            )

    out_project(0, mate, part_out)
    part_copy(0).start()
    out_project(0, h, part_own)
    landed(8)
    landed(9)
    for j in range(1, routers):
        out_project(j, mate, part_out)
        part_copy(j).start()
    for j in range(1, routers):
        out_project(j, h, part_own)
    c_one.wait()
    for j in range(routers):
        part_copy(j).wait_recv()

    sources_tile = tile_slots // CAP
    two = jnp.broadcast_to(w_two_ref[...], (8, w_two_ref.shape[1]))

    @pl.loop(0, half_tiles)
    def _(i):
        span = pl.ds(pl.multiple_of(i * tile, tile), tile)
        x = x_tile(h * half_tiles + i).astype(F32)
        mixed = []
        for a in range(routers):
            j = lax.rem(r - a + routers, routers)
            mixed.append(part_own[j, span, :] + part_in[j, span, :])
        residual = x + jnp.concatenate(mixed, axis=1)
        norm = lax.rsqrt(jnp.sum(residual * residual, axis=1, keepdims=True) / model + EPSILON)
        normed = (residual * norm * mlp_gain_ref[...].astype(F32)).astype(BF16)
        hidden = silu(jnp.dot(normed, w_one_v[...], preferred_element_type=F32)).astype(BF16)
        found = lax.dot_general(two, hidden, (((1,), (1,)), ((), ())), preferred_element_type=F32)
        for s in range(sources_tile):
            sc_out[i * sources_tile + s] = found[:, s * CAP * width : (s + 1) * CAP * width]

    mine = users // heads

    def score_copy(i, e, owner, sem):
        return pltpu.make_async_remote_copy(
            src_ref=sc_out.at[i],
            dst_ref=ret.at[owner],
            send_sem=sc_send.at[i, e],
            recv_sem=sc_recv.at[sem],
            device_id={"users": h * mine + i, "heads": e},
            device_id_type=MESH,
        )

    for i in range(mine):
        target = h * mine + i
        for e in range(heads):
            itself = (target == me) & (h == e)

            @pl.when(jnp.logical_not(itself))
            def _():
                score_copy(i, e, me, me).start()

            @pl.when(itself)
            def _():
                ret[me] = sc_out[i]

    handler = me // mine
    for d in range(users):

        @pl.when(jnp.logical_not((d == me) & (h == handler)))
        def _():
            score_copy(0, 0, d, d).wait_recv()

    position = lax.broadcasted_iota(jnp.int32, (1, width), 1)
    for b in range(blocks):
        tile_in = ret[owners[b]]
        line = tile_in[0:1, 0:width]
        for cap in range(1, CAP):
            line = jnp.where(ranks[b] == cap, tile_in[0:1, cap * width : (cap + 1) * width], line)
        out_ref[b : b + 1, :] = jnp.where(position < fill_ref[b], line, 0.0)

    for t in range(len(pieces)):
        for j in range(1, routers):
            x_copy(j, t, r).wait_send()
            for i in range(1, groups):
                y_copy(i, j, t, g).wait_send()
    for k in range(1, users):
        z_copy(k, me).wait_send()
        m_copy(k, me).wait_send()
        relay_copy(k, h).wait_send()
    stat_copy.wait_send()
    for j in range(routers):
        part_copy(j).wait_send()
    for i in range(mine):
        for e in range(heads):

            @pl.when(jnp.logical_not((h * mine + i == me) & (h == e)))
            def _():
                score_copy(i, e, me, me).wait_send()


def local(
    sizes,
    items,
    block_owner,
    block_user,
    block_fill,
    prefix_keys,
    prefix_values,
    w_in,
    attn_gain,
    w_o,
    mlp_gain,
    w_one,
    w_two,
):
    groups, users, routers, heads = sizes
    blocks, width, model = items.shape
    projections, depth, half_width = w_in.shape
    slots = users * CAP
    rows = slots * width
    half = rows // heads
    out_cols = w_o.shape[1]
    cached, per_user, _ = prefix_keys.shape
    positions = cached * per_user
    pieces = 5 * SUB
    dma = pltpu.SemaphoreType.DMA
    hbm = pl.BlockSpec(memory_space=pl.ANY)
    vmem = pl.BlockSpec(memory_space=pltpu.VMEM)
    smem = pl.BlockSpec(memory_space=pltpu.SMEM)
    scratch = [
        pltpu.VMEM((blocks, width, model), BF16),
        pltpu.VMEM((users, CAP, width // heads, model), BF16),
        pltpu.VMEM((slots, width, model), BF16),
        pltpu.VMEM((users, 8, positions), F32),
        pltpu.VMEM((users, 8, positions), F32),
        pltpu.VMEM(prefix_keys.shape, BF16),
        pltpu.VMEM(prefix_values.shape, BF16),
        pltpu.VMEM((projections, routers, depth, half_width), BF16),
        pltpu.VMEM((routers, half_width, out_cols), BF16),
        pltpu.VMEM(w_one.shape, BF16),
        pltpu.VMEM((rows, half_width), BF16),
        pltpu.VMEM((rows, half_width), F32),
        pltpu.VMEM((rows, half_width), F32),
        pltpu.VMEM((rows, half_width), F32),
        pltpu.VMEM((rows, half_width), F32),
        pltpu.VMEM((rows, half_width), BF16),
        pltpu.VMEM((rows, 128), F32),
        pltpu.VMEM((rows, 128), F32),
        pltpu.VMEM((routers, half, out_cols), F32),
        pltpu.VMEM((routers, half, out_cols), F32),
        pltpu.VMEM((routers, half, out_cols), F32),
        pltpu.VMEM((users // heads, 8, CAP * width), F32),
        pltpu.VMEM((users, 8, CAP * width), F32),
        dma((6,)),
        dma((users,)),
        dma((users,)),
        dma((users,)),
        dma((users,)),
        dma((users,)),
        dma((users,)),
        dma((routers, pieces)),
        dma((routers, pieces)),
        dma((groups, routers, pieces)),
        dma((groups, routers, pieces)),
        dma((2,)),
        dma((routers,)),
        dma((routers,)),
        dma((users // heads, heads)),
        dma((users,)),
    ]
    return pl.pallas_call(
        functools.partial(scorer, sizes),
        out_shape=jax.ShapeDtypeStruct((blocks, width), F32),
        in_specs=[hbm, smem, smem, smem, hbm, hbm, hbm, vmem, hbm, vmem, hbm, vmem],
        out_specs=vmem,
        scratch_shapes=scratch,
        compiler_params=pltpu.CompilerParams(
            collective_id=0, has_side_effects=True, vmem_limit_bytes=62 * 1024 * 1024
        ),
    )(
        items,
        block_owner,
        block_user,
        block_fill,
        prefix_keys,
        prefix_values,
        w_in,
        attn_gain.reshape(1, -1),
        w_o,
        mlp_gain.reshape(1, -1),
        w_one,
        w_two.reshape(1, -1),
    )


def solution(mesh):
    placed = (
        P(("groups", "users", "routers"), None, None),
        P(("groups", "users", "routers"), None),
        P(("groups", "users", "routers")),
        P(("groups", "users", "routers")),
        P(("groups", "users"), None, "heads"),
        P(("groups", "users"), None, "heads"),
        P(None, "routers", "heads"),
        P("heads"),
        P("heads", "routers"),
        P(),
        P(),
        P(),
    )
    sizes = tuple(mesh.shape[name] for name in ("groups", "users", "routers", "heads"))
    return jax.shard_map(
        functools.partial(local, sizes),
        mesh=mesh,
        in_specs=placed,
        out_specs=P(("groups", "users", "routers"), None),
        check_vma=False,
    )
```

```python
import functools

import jax
import jax.numpy as jnp
from jax import lax
from jax.experimental import pallas as pl
from jax.experimental.pallas import tpu as pltpu
from jax.sharding import PartitionSpec as P

HEAD_DIM = 128
CAP = 2
EPSILON = 1e-05
F32 = jnp.float32
BF16 = jnp.bfloat16
MESH = pl.DeviceIdType.MESH


def silu(v):
    return 0.5 * v * (1.0 + jnp.tanh(0.5 * v))


def scorer(
    sizes,
    items_ref,
    owner_ref,
    user_ref,
    fill_ref,
    keys_ref,
    values_ref,
    w_in_ref,
    attn_gain_ref,
    w_o_ref,
    mlp_gain_ref,
    w_one_ref,
    w_two_ref,
    out_ref,
    items_v,
    out_slots,
    x_all,
    mask_out,
    mask_all,
    keys_v,
    values_v,
    w_all,
    wo_all,
    w_one_v,
    q_v,
    sk_v,
    sv_v,
    gates_v,
    att_v,
    gated_v,
    stat_out,
    stat_in,
    part_out,
    part_own,
    part_in,
    sc_out,
    ret,
    local_sem,
    z_send,
    z_recv,
    m_send,
    m_recv,
    rel_send,
    rel_recv,
    x_send,
    x_recv,
    y_send,
    y_recv,
    w_send,
    w_recv,
    st_sem,
    po_send,
    po_recv,
    sc_send,
    sc_recv,
):
    groups, users, routers, heads = sizes
    g = lax.axis_index("groups")
    me = lax.axis_index("users")
    r = lax.axis_index("routers")
    h = lax.axis_index("heads")
    mate = 1 - h
    blocks, width, model = items_v.shape
    slots = x_all.shape[0]
    half_width = q_v.shape[1]
    heads_here = half_width // HEAD_DIM
    hd_all = half_width * heads
    rows = slots * width
    depth = w_all.shape[2]
    out_cols = wo_all.shape[2]
    wh = width // heads
    scale = HEAD_DIM ** (-0.5)
    positions = keys_v.shape[0] * keys_v.shape[1]
    per_user = keys_v.shape[1]

    c_items = pltpu.make_async_copy(items_ref, items_v, local_sem.at[0])
    c_items.start()

    barrier = pltpu.get_barrier_semaphore()
    count = 0
    for j in range(1, routers):
        pl.semaphore_signal(
            barrier, inc=1, device_id={"routers": lax.rem(r + j, routers)}, device_id_type=MESH
        )
        count += 1
    for i in range(1, groups):
        pl.semaphore_signal(
            barrier, inc=1, device_id={"groups": lax.rem(g + i, groups)}, device_id_type=MESH
        )
        count += 1
    pl.semaphore_signal(barrier, inc=1, device_id={"heads": mate}, device_id_type=MESH)
    count += 1
    for k in range(1, users):
        for e in range(heads):
            pl.semaphore_signal(
                barrier,
                inc=1,
                device_id={"users": lax.rem(me + k, users), "heads": e},
                device_id_type=MESH,
            )
            count += 1
    c_keys = pltpu.make_async_copy(keys_ref, keys_v, local_sem.at[1])
    c_values = pltpu.make_async_copy(values_ref, values_v, local_sem.at[2])
    c_win = pltpu.make_async_copy(w_in_ref, w_all.at[:, r], local_sem.at[3])
    c_wo = pltpu.make_async_copy(w_o_ref, wo_all.at[r], local_sem.at[4])
    c_one = pltpu.make_async_copy(w_one_ref, w_one_v, local_sem.at[5])
    pl.semaphore_wait(barrier, count)

    pieces = [(p, kind) for p in range(5) for kind in range(2)]
    parity = lax.rem(me, 2)
    pair = me + 1 - 2 * parity

    def piece_rows(length, kind, owner_group, owner_parity):
        if kind == 0:
            share = length // 4 // groups
            return pl.ds(pl.multiple_of((owner_group * 2 + owner_parity) * share, share), share)
        share = length // 2 // groups
        return pl.ds(pl.multiple_of(length // 2 + owner_group * share, share), share)

    def weight_slot(owner_router, owner_group, owner_parity, t):
        p, kind = pieces[t]
        if p < 4:
            return w_all.at[p, owner_router, piece_rows(depth, kind, owner_group, owner_parity), :]
        return wo_all.at[owner_router, piece_rows(half_width, kind, owner_group, owner_parity), :]

    def x_copy(j, t, source_router):
        p, kind = pieces[t]
        if p < 4:
            src = w_in_ref.at[p, piece_rows(depth, kind, g, parity), :]
        else:
            src = w_o_ref.at[piece_rows(half_width, kind, g, parity), :]
        return pltpu.make_async_remote_copy(
            src_ref=src,
            dst_ref=weight_slot(source_router, g, parity, t),
            send_sem=x_send.at[j, t],
            recv_sem=x_recv.at[j, t],
            device_id={"routers": lax.rem(r + j, routers)},
            device_id_type=MESH,
        )

    def y_copy(i, j, t, owner_group):
        spot = weight_slot(lax.rem(r - j + routers, routers), owner_group, parity, t)
        return pltpu.make_async_remote_copy(
            src_ref=spot,
            dst_ref=spot,
            send_sem=y_send.at[i, j, t],
            recv_sem=y_recv.at[i, j, t],
            device_id={"groups": lax.rem(g + i, groups)},
            device_id_type=MESH,
        )

    def pair_copy(i, j, p, owner_parity):
        spot = weight_slot(
            lax.rem(r - j + routers, routers), lax.rem(g - i + groups, groups), owner_parity, 2 * p
        )
        return pltpu.make_async_remote_copy(
            src_ref=spot,
            dst_ref=spot,
            send_sem=w_send.at[i, j, p],
            recv_sem=w_recv.at[i, j, p],
            device_id={"users": pair},
            device_id_type=MESH,
        )

    for t in range(len(pieces)):
        for j in range(1, routers):
            x_copy(j, t, r).start()
    for c in (c_win, c_keys, c_values, c_wo, c_one):
        c.start()

    owners = [owner_ref[b] for b in range(blocks)]
    ranks = []
    for b in range(blocks):
        rank = jnp.int32(0)
        for a in range(b):
            rank = rank + jnp.where(owners[a] == owners[b], 1, 0)
        ranks.append(rank)

    def slot_source(dest, cap):
        index, user = jnp.int32(0), jnp.int32(-1)
        for b in range(blocks):
            hit = (owners[b] == dest) & (ranks[b] == cap)
            index = jnp.where(hit, b, index)
            user = jnp.where(hit, user_ref[b], user)
        return index, user

    lane_user = lax.broadcasted_iota(jnp.int32, (1, positions), 1) // per_user
    mask_copies, item_copies = {}, {}

    def z_copy(k, source):
        return pltpu.make_async_remote_copy(
            src_ref=out_slots.at[k],
            dst_ref=x_all.at[pl.ds(source * CAP, CAP), pl.ds(pl.multiple_of(h * wh, wh), wh), :],
            send_sem=z_send.at[k],
            recv_sem=z_recv.at[k],
            device_id={"users": lax.rem(me + k, users)},
            device_id_type=MESH,
        )

    def m_copy(k, source):
        return pltpu.make_async_remote_copy(
            src_ref=mask_out.at[k],
            dst_ref=mask_all.at[source],
            send_sem=m_send.at[k],
            recv_sem=m_recv.at[k],
            device_id={"users": lax.rem(me + k, users)},
            device_id_type=MESH,
        )

    def relay_copy(k, part):
        source = lax.rem(me - k + users, users)
        spot = x_all.at[pl.ds(source * CAP, CAP), pl.ds(pl.multiple_of(part * wh, wh), wh), :]
        return pltpu.make_async_remote_copy(
            src_ref=spot,
            dst_ref=spot,
            send_sem=rel_send.at[k],
            recv_sem=rel_recv.at[k],
            device_id={"heads": mate},
            device_id_type=MESH,
        )

    c_items.wait()
    for k in list(range(1, users)) + [0]:
        dest = lax.rem(me + k, users)
        for cap in range(CAP):
            index, user = slot_source(dest, cap)
            line = jnp.where(lane_user == user, 1.0, 0.0).astype(F32)
            if k == 0:
                x_all[me * CAP + cap] = items_v[index]
                mask_all[me, cap : cap + 1, :] = line
            else:
                out_slots[k, cap] = items_v[index, pl.ds(pl.multiple_of(h * wh, wh), wh), :]
                mask_out[k, cap : cap + 1, :] = line
        if k:
            z_copy(k, me).start()
            m_copy(k, me).start()

    def forward(p, kind):
        t = 2 * p + kind
        for j in range(1, routers):
            x_copy(j, t, lax.rem(r - j + routers, routers)).wait_recv()
            for i in range(1, groups):
                y_copy(i, j, t, g).start()
            if kind == 0:
                pair_copy(0, j, p, parity).start()

    def y_landed(t):
        for j in range(1, routers):
            for i in range(1, groups):
                y_copy(i, j, t, lax.rem(g - i + groups, groups)).wait_recv()
                if t % 2 == 0:
                    pair_copy(i, j, t // 2, parity).start()

    def landed(p):
        y_landed(2 * p + 1)
        for j in range(1, routers):
            for i in range(groups):
                pair_copy(i, j, p, 1 - parity).wait_recv()

    def items_landed():
        for k in range(1, users):
            z_copy(k, lax.rem(me - k + users, users)).wait_recv()
            relay_copy(k, h).start()
        for k in range(1, users):
            m_copy(k, lax.rem(me - k + users, users)).wait_recv()
            relay_copy(k, mate).wait_recv()

    for p in range(3):
        with jax.named_scope(f"fwd{p}"):
            forward(p, 0)
            forward(p, 1)
            y_landed(2 * p)
    with jax.named_scope("items"):
        items_landed()
        c_win.wait()

    tile = 4 * width
    tile_slots = 4
    tiles = rows // tile

    def x_tile(i):
        return x_all[pl.ds(i * tile_slots, tile_slots)].reshape(tile, model)

    def project(p, target):
        @pl.loop(0, tiles)
        def _(i):
            x = x_tile(i)
            total = jnp.zeros((tile, half_width), F32)
            for a in range(routers):
                total = total + jnp.dot(
                    x[:, a * depth : (a + 1) * depth],
                    w_all[p, a],
                    preferred_element_type=F32,
                )
            target[pl.ds(pl.multiple_of(i * tile, tile), tile), :] = silu(total).astype(target.dtype)

    with jax.named_scope("land0"):
        landed(0)
    with jax.named_scope("proj0"):
        project(0, q_v)
    with jax.named_scope("fwd3a"):
        forward(3, 0)
    c_keys.wait()
    c_values.wait()

    def attend(i):
        span = pl.ds(pl.multiple_of(i * tile, tile), tile)
        for e in range(heads_here):
            cols = slice(e * HEAD_DIM, (e + 1) * HEAD_DIM)
            raw = lax.dot_general(
                q_v[span, cols],
                keys_v[:, :, cols].reshape(positions, HEAD_DIM),
                (((1,), (1,)), ((), ())),
                preferred_element_type=F32,
            )
            weights = silu(raw * scale)
            parts = []
            for s in range(tile_slots):
                line = mask_all[i * (tile_slots // CAP) + s // CAP, s % CAP : s % CAP + 1, :]
                parts.append(weights[s * width : (s + 1) * width] * line)
            weights = jnp.concatenate(parts, axis=0).astype(BF16)
            att_v[span, cols] = (
                jnp.dot(
                    weights,
                    values_v[:, :, cols].reshape(positions, HEAD_DIM),
                    preferred_element_type=F32,
                )
                .astype(BF16)
                .astype(F32)
            )

    with jax.named_scope("attend0"):
        pl.loop(0, tiles // 2)(attend)
    with jax.named_scope("fwd3b"):
        forward(3, 1)
        y_landed(6)
    with jax.named_scope("attend1"):
        pl.loop(tiles // 2, tiles)(attend)
    with jax.named_scope("land1"):
        landed(1)
    with jax.named_scope("proj1"):
        project(1, sk_v)
    with jax.named_scope("fwd4a"):
        forward(4, 0)
    with jax.named_scope("land2"):
        landed(2)
    with jax.named_scope("proj2"):
        project(2, sv_v)

    lane = lax.broadcasted_iota(jnp.int32, (tile, 128), 1)

    @pl.loop(0, tiles)
    def _(i):
        span = pl.ds(pl.multiple_of(i * tile, tile), tile)
        total = jnp.zeros((tile, 1), F32)
        square = jnp.zeros((tile, 1), F32)
        for e in range(heads_here):
            cols = slice(e * HEAD_DIM, (e + 1) * HEAD_DIM)
            own = jnp.sum(q_v[span, cols].astype(F32) * sk_v[span, cols], axis=1, keepdims=True)
            att = att_v[span, cols] + silu(own * scale) * sv_v[span, cols]
            att_v[span, cols] = att
            total = total + jnp.sum(att, axis=1, keepdims=True)
            square = square + jnp.sum(att * att, axis=1, keepdims=True)
        stat_out[span, :] = jnp.where(lane == 0, total, square)

    stat_copy = pltpu.make_async_remote_copy(
        src_ref=stat_out,
        dst_ref=stat_in,
        send_sem=st_sem.at[0],
        recv_sem=st_sem.at[1],
        device_id={"heads": mate},
        device_id_type=MESH,
    )
    stat_copy.start()
    with jax.named_scope("fwd4b"):
        forward(4, 1)
        y_landed(8)
    with jax.named_scope("land3"):
        landed(3)
    with jax.named_scope("proj3"):
        project(3, gates_v)
    with jax.named_scope("statwait"):
        stat_copy.wait_recv()

    @pl.loop(0, tiles)
    def _(i):
        span = pl.ds(pl.multiple_of(i * tile, tile), tile)
        both = stat_out[span, :] + stat_in[span, :]
        mean = both[:, 0:1] / hd_all
        var = both[:, 1:2] / hd_all - mean * mean
        gated_v[span, :] = (
            (att_v[span, :] - mean)
            * lax.rsqrt(var + EPSILON)
            * attn_gain_ref[...].astype(F32).reshape(1, -1)
            * gates_v[span, :]
        ).astype(BF16)

    half = rows // heads
    half_tiles = half // tile
    c_wo.wait()

    def part_copy(j):
        return pltpu.make_async_remote_copy(
            src_ref=part_out.at[j],
            dst_ref=part_in.at[j],
            send_sem=po_send.at[j],
            recv_sem=po_recv.at[j],
            device_id={"heads": mate},
            device_id_type=MESH,
        )

    def out_project(j, row_half, target):
        a = lax.rem(r - j + routers, routers)

        @pl.loop(0, half_tiles)
        def _(i):
            src = pl.ds(pl.multiple_of(row_half * half + i * tile, tile), tile)
            target[j, pl.ds(pl.multiple_of(i * tile, tile), tile), :] = jnp.dot(
                gated_v[src, :], wo_all[a], preferred_element_type=F32
            )

    out_project(0, mate, part_out)
    part_copy(0).start()
    out_project(0, h, part_own)
    with jax.named_scope("land4"):
        landed(4)
    for j in range(1, routers):
        out_project(j, mate, part_out)
        part_copy(j).start()
    for j in range(1, routers):
        out_project(j, h, part_own)
    c_one.wait()
    with jax.named_scope("partwait"):
        for j in range(routers):
            part_copy(j).wait_recv()

    sources_tile = tile_slots // CAP
    two = jnp.broadcast_to(w_two_ref[...].astype(F32).reshape(1, -1), (8, w_two_ref.shape[0])).astype(BF16)

    @pl.loop(0, half_tiles)
    def _(i):
        span = pl.ds(pl.multiple_of(i * tile, tile), tile)
        x = x_tile(h * half_tiles + i).astype(F32)
        mixed = []
        for a in range(routers):
            j = lax.rem(r - a + routers, routers)
            mixed.append(part_own[j, span, :] + part_in[j, span, :])
        residual = x + jnp.concatenate(mixed, axis=1)
        norm = lax.rsqrt(jnp.sum(residual * residual, axis=1, keepdims=True) / model + EPSILON)
        normed = (residual * norm * mlp_gain_ref[...].astype(F32).reshape(1, -1)).astype(BF16)
        hidden = silu(jnp.dot(normed, w_one_v[...], preferred_element_type=F32)).astype(BF16)
        found = lax.dot_general(two, hidden, (((1,), (1,)), ((), ())), preferred_element_type=F32)
        for s in range(sources_tile):
            sc_out[i * sources_tile + s] = found[:, s * CAP * width : (s + 1) * CAP * width]

    mine = users // heads

    def score_copy(i, e, owner, sem):
        return pltpu.make_async_remote_copy(
            src_ref=sc_out.at[i],
            dst_ref=ret.at[owner],
            send_sem=sc_send.at[i, e],
            recv_sem=sc_recv.at[sem],
            device_id={"users": h * mine + i, "heads": e},
            device_id_type=MESH,
        )

    for i in range(mine):
        target = h * mine + i
        for e in range(heads):
            itself = (target == me) & (h == e)

            @pl.when(jnp.logical_not(itself))
            def _():
                score_copy(i, e, me, me).start()

            @pl.when(itself)
            def _():
                ret[me] = sc_out[i]

    handler = me // mine
    with jax.named_scope("scorewait"):
        for d in range(users):

            @pl.when(jnp.logical_not((d == me) & (h == handler)))
            def _():
                score_copy(0, 0, d, d).wait_recv()

    position = lax.broadcasted_iota(jnp.int32, (1, width), 1)
    for b in range(blocks):
        tile_in = ret[owners[b]]
        line = tile_in[0:1, 0:width]
        for cap in range(1, CAP):
            line = jnp.where(ranks[b] == cap, tile_in[0:1, cap * width : (cap + 1) * width], line)
        out_ref[b : b + 1, :] = jnp.where(position < fill_ref[b], line, 0.0)

    for t in range(len(pieces)):
        for j in range(1, routers):
            x_copy(j, t, r).wait_send()
            for i in range(1, groups):
                y_copy(i, j, t, g).wait_send()
    for p in range(5):
        for j in range(1, routers):
            for i in range(groups):
                pair_copy(i, j, p, parity).wait_send()
    for k in range(1, users):
        z_copy(k, me).wait_send()
        m_copy(k, me).wait_send()
        relay_copy(k, h).wait_send()
    stat_copy.wait_send()
    for j in range(routers):
        part_copy(j).wait_send()
    for i in range(mine):
        for e in range(heads):

            @pl.when(jnp.logical_not((h * mine + i == me) & (h == e)))
            def _():
                score_copy(i, e, me, me).wait_send()


def local(
    sizes,
    items,
    block_owner,
    block_user,
    block_fill,
    prefix_keys,
    prefix_values,
    w_in,
    attn_gain,
    w_o,
    mlp_gain,
    w_one,
    w_two,
):
    groups, users, routers, heads = sizes
    blocks, width, model = items.shape
    projections, depth, half_width = w_in.shape
    slots = users * CAP
    rows = slots * width
    half = rows // heads
    out_cols = w_o.shape[1]
    cached, per_user, _ = prefix_keys.shape
    positions = cached * per_user
    pieces = 10
    dma = pltpu.SemaphoreType.DMA
    hbm = pl.BlockSpec(memory_space=pl.ANY)
    vmem = pl.BlockSpec(memory_space=pltpu.VMEM)
    smem = pl.BlockSpec(memory_space=pltpu.SMEM)
    scratch = [
        pltpu.VMEM((blocks, width, model), BF16),
        pltpu.VMEM((users, CAP, width // heads, model), BF16),
        pltpu.VMEM((slots, width, model), BF16),
        pltpu.VMEM((users, 8, positions), F32),
        pltpu.VMEM((users, 8, positions), F32),
        pltpu.VMEM(prefix_keys.shape, BF16),
        pltpu.VMEM(prefix_values.shape, BF16),
        pltpu.VMEM((projections, routers, depth, half_width), BF16),
        pltpu.VMEM((routers, half_width, out_cols), BF16),
        pltpu.VMEM(w_one.shape, BF16),
        pltpu.VMEM((rows, half_width), BF16),
        pltpu.VMEM((rows, half_width), F32),
        pltpu.VMEM((rows, half_width), F32),
        pltpu.VMEM((rows, half_width), F32),
        pltpu.VMEM((rows, half_width), F32),
        pltpu.VMEM((rows, half_width), BF16),
        pltpu.VMEM((rows, 128), F32),
        pltpu.VMEM((rows, 128), F32),
        pltpu.VMEM((routers, half, out_cols), F32),
        pltpu.VMEM((routers, half, out_cols), F32),
        pltpu.VMEM((routers, half, out_cols), F32),
        pltpu.VMEM((users // heads, 8, CAP * width), F32),
        pltpu.VMEM((users, 8, CAP * width), F32),
        dma((6,)),
        dma((users,)),
        dma((users,)),
        dma((users,)),
        dma((users,)),
        dma((users,)),
        dma((users,)),
        dma((routers, pieces)),
        dma((routers, pieces)),
        dma((groups, routers, pieces)),
        dma((groups, routers, pieces)),
        dma((groups, routers, 5)),
        dma((groups, routers, 5)),
        dma((2,)),
        dma((routers,)),
        dma((routers,)),
        dma((users // heads, heads)),
        dma((users,)),
    ]
    return pl.pallas_call(
        functools.partial(scorer, sizes),
        out_shape=jax.ShapeDtypeStruct((blocks, width), F32),
        in_specs=[hbm, smem, smem, smem, hbm, hbm, hbm, vmem, hbm, vmem, hbm, vmem],
        out_specs=vmem,
        scratch_shapes=scratch,
        compiler_params=pltpu.CompilerParams(
            collective_id=0, has_side_effects=True, vmem_limit_bytes=62 * 1024 * 1024
        ),
    )(
        items,
        block_owner.reshape(-1),
        block_user,
        block_fill,
        prefix_keys,
        prefix_values,
        w_in,
        attn_gain,
        w_o,
        mlp_gain,
        w_one,
        w_two,
    )


def solution(mesh):
    placed = (
        P(("groups", "users", "routers"), None, None),
        P(("groups", "users", "routers"), None),
        P(("groups", "users", "routers")),
        P(("groups", "users", "routers")),
        P(("groups", "users"), None, "heads"),
        P(("groups", "users"), None, "heads"),
        P(None, "routers", "heads"),
        P("heads"),
        P("heads", "routers"),
        P(),
        P(),
        P(),
    )
    sizes = tuple(mesh.shape[name] for name in ("groups", "users", "routers", "heads"))
    return jax.shard_map(
        functools.partial(local, sizes),
        mesh=mesh,
        in_specs=placed,
        out_specs=P(("groups", "users", "routers"), None),
        check_vma=False,
    )
```

```python
import functools
import math

import jax
import jax.numpy as jnp
from jax import lax
from jax.experimental import pallas as pl
from jax.experimental.pallas import tpu as pltpu
from jax.sharding import PartitionSpec as P

HEAD_DIM = 128
CAP = 2
EPSILON = 1e-05
TREE_EIGHTHS = (0, 5, 5, 5, 4)
PARTS = (4, 1, 1, 1, 4)
ORDER = (
    [(0, "g", part) for part in range(PARTS[0])]
    + [(1, "t", 0), (2, "t", 0), (1, "g", 0), (3, "t", 0), (4, "t", 0), (2, "g", 0), (3, "g", 0)]
    + [(4, "g", part) for part in range(PARTS[4])]
)
F32 = jnp.float32
BF16 = jnp.bfloat16
MESH = pl.DeviceIdType.MESH


def silu(v):
    return 0.5 * v * (1.0 + jnp.tanh(0.5 * v))


def scorer(
    sizes,
    items_ref,
    owner_ref,
    user_ref,
    fill_ref,
    keys_ref,
    values_ref,
    w_in_ref,
    attn_gain_ref,
    w_o_ref,
    mlp_gain_ref,
    w_one_ref,
    w_two_ref,
    out_ref,
    items_v,
    out_slots,
    x_all,
    mask_out,
    mask_all,
    keys_v,
    values_v,
    w_all,
    wo_all,
    w_one_v,
    q_v,
    own_v,
    att_v,
    gated_v,
    stat_out,
    stat_in,
    part_out,
    part_own,
    part_in,
    sc_out,
    ret,
    local_sem,
    z_send,
    z_recv,
    m_send,
    m_recv,
    rel_send,
    rel_recv,
    x_send,
    x_recv,
    y_send,
    y_recv,
    w_send,
    w_recv,
    st_sem,
    po_send,
    po_recv,
    sc_send,
    sc_recv,
):
    groups, users, routers, heads = sizes
    g = lax.axis_index("groups")
    me = lax.axis_index("users")
    r = lax.axis_index("routers")
    h = lax.axis_index("heads")
    mate = 1 - h
    blocks, width, model = items_v.shape
    slots = x_all.shape[0]
    half_width = q_v.shape[1]
    heads_here = half_width // HEAD_DIM
    hd_all = half_width * heads
    rows = slots * width
    depth = w_all.shape[2]
    out_cols = wo_all.shape[2]
    wh = width // heads
    scale = HEAD_DIM ** (-0.5)
    positions = keys_v.shape[0] * keys_v.shape[1]
    per_user = keys_v.shape[1]

    c_items = pltpu.make_async_copy(items_ref, items_v, local_sem.at[0])
    c_items.start()

    barrier = pltpu.get_barrier_semaphore()
    count = 0
    for j in range(1, routers):
        pl.semaphore_signal(
            barrier, inc=1, device_id={"routers": lax.rem(r + j, routers)}, device_id_type=MESH
        )
        count += 1
    for i in range(1, groups):
        pl.semaphore_signal(
            barrier, inc=1, device_id={"groups": lax.rem(g + i, groups)}, device_id_type=MESH
        )
        count += 1
    pl.semaphore_signal(barrier, inc=1, device_id={"heads": mate}, device_id_type=MESH)
    count += 1
    for k in range(1, users):
        for e in range(heads):
            pl.semaphore_signal(
                barrier,
                inc=1,
                device_id={"users": lax.rem(me + k, users), "heads": e},
                device_id_type=MESH,
            )
            count += 1
    c_keys = pltpu.make_async_copy(keys_ref, keys_v, local_sem.at[1])
    c_values = pltpu.make_async_copy(values_ref, values_v, local_sem.at[2])
    c_win = pltpu.make_async_copy(w_in_ref, w_all.at[:, r], local_sem.at[3])
    c_wo = pltpu.make_async_copy(w_o_ref, wo_all.at[r], local_sem.at[4])
    c_one = pltpu.make_async_copy(w_one_ref, w_one_v, local_sem.at[5])
    pl.semaphore_wait(barrier, count)

    pieces = ORDER
    number = {piece: t for t, piece in enumerate(pieces)}
    parity = lax.rem(me, 2)
    pair = me + 1 - 2 * parity

    def piece_rows(p, kind, part, owner_group, owner_parity):
        length = depth if p < 4 else half_width
        tree = length * TREE_EIGHTHS[p] // 8 // (2 * groups) // 16 * 16
        if kind == "t":
            return pl.ds(pl.multiple_of((owner_group * 2 + owner_parity) * tree, tree), tree)
        direct = length // groups - 2 * tree
        share = direct // PARTS[p]
        start = 2 * groups * tree + owner_group * direct + part * share
        return pl.ds(pl.multiple_of(start, math.gcd(share, 16)), share)

    def weight_slot(owner_router, owner_group, owner_parity, t):
        p, kind, part = pieces[t]
        span = piece_rows(p, kind, part, owner_group, owner_parity)
        if p < 4:
            return w_all.at[p, owner_router, span, :]
        return wo_all.at[owner_router, span, :]

    def x_copy(j, t, source_router):
        p, kind, part = pieces[t]
        span = piece_rows(p, kind, part, g, parity)
        src = w_in_ref.at[p, span, :] if p < 4 else w_o_ref.at[span, :]
        return pltpu.make_async_remote_copy(
            src_ref=src,
            dst_ref=weight_slot(source_router, g, parity, t),
            send_sem=x_send.at[j, t],
            recv_sem=x_recv.at[j, t],
            device_id={"routers": lax.rem(r + j, routers)},
            device_id_type=MESH,
        )

    def y_copy(i, j, t, owner_group):
        spot = weight_slot(lax.rem(r - j + routers, routers), owner_group, parity, t)
        return pltpu.make_async_remote_copy(
            src_ref=spot,
            dst_ref=spot,
            send_sem=y_send.at[i, j, t],
            recv_sem=y_recv.at[i, j, t],
            device_id={"groups": lax.rem(g + i, groups)},
            device_id_type=MESH,
        )

    def pair_copy(i, j, p, owner_parity):
        spot = weight_slot(
            lax.rem(r - j + routers, routers),
            lax.rem(g - i + groups, groups),
            owner_parity,
            number[p, "t", 0],
        )
        return pltpu.make_async_remote_copy(
            src_ref=spot,
            dst_ref=spot,
            send_sem=w_send.at[i, j, p],
            recv_sem=w_recv.at[i, j, p],
            device_id={"users": pair},
            device_id_type=MESH,
        )

    for t in range(len(pieces)):
        for j in range(1, routers):
            x_copy(j, t, r).start()
    for c in (c_win, c_keys, c_values, c_wo, c_one):
        c.start()

    owners = [owner_ref[b] for b in range(blocks)]
    ranks = []
    for b in range(blocks):
        rank = jnp.int32(0)
        for a in range(b):
            rank = rank + jnp.where(owners[a] == owners[b], 1, 0)
        ranks.append(rank)

    def slot_source(dest, cap):
        index, user = jnp.int32(0), jnp.int32(-1)
        for b in range(blocks):
            hit = (owners[b] == dest) & (ranks[b] == cap)
            index = jnp.where(hit, b, index)
            user = jnp.where(hit, user_ref[b], user)
        return index, user

    lane_user = lax.broadcasted_iota(jnp.int32, (1, positions), 1) // per_user
    mask_copies, item_copies = {}, {}

    def z_copy(k, source):
        return pltpu.make_async_remote_copy(
            src_ref=out_slots.at[k],
            dst_ref=x_all.at[pl.ds(source * CAP, CAP), pl.ds(pl.multiple_of(h * wh, wh), wh), :],
            send_sem=z_send.at[k],
            recv_sem=z_recv.at[k],
            device_id={"users": lax.rem(me + k, users)},
            device_id_type=MESH,
        )

    def m_copy(k, source):
        return pltpu.make_async_remote_copy(
            src_ref=mask_out.at[k],
            dst_ref=mask_all.at[source],
            send_sem=m_send.at[k],
            recv_sem=m_recv.at[k],
            device_id={"users": lax.rem(me + k, users)},
            device_id_type=MESH,
        )

    def relay_copy(k, part):
        source = lax.rem(me - k + users, users)
        spot = x_all.at[pl.ds(source * CAP, CAP), pl.ds(pl.multiple_of(part * wh, wh), wh), :]
        return pltpu.make_async_remote_copy(
            src_ref=spot,
            dst_ref=spot,
            send_sem=rel_send.at[k],
            recv_sem=rel_recv.at[k],
            device_id={"heads": mate},
            device_id_type=MESH,
        )

    c_items.wait()
    for k in list(range(1, users)) + [0]:
        dest = lax.rem(me + k, users)
        for cap in range(CAP):
            index, user = slot_source(dest, cap)
            line = jnp.where(lane_user == user, 1.0, 0.0).astype(F32)
            if k == 0:
                x_all[me * CAP + cap] = items_v[index]
                mask_all[me, cap : cap + 1, :] = line
            else:
                out_slots[k, cap] = items_v[index, pl.ds(pl.multiple_of(h * wh, wh), wh), :]
                mask_out[k, cap : cap + 1, :] = line
        if k:
            z_copy(k, me).start()
            m_copy(k, me).start()

    def forward(p, kind, part=0):
        t = number[p, kind, part]
        for j in range(1, routers):
            x_copy(j, t, lax.rem(r - j + routers, routers)).wait_recv()
            for i in range(1, groups):
                y_copy(i, j, t, g).start()
            if kind == "t":
                pair_copy(0, j, p, parity).start()

    def y_landed(p, kind, part=0):
        t = number[p, kind, part]
        for j in range(1, routers):
            for i in range(1, groups):
                y_copy(i, j, t, lax.rem(g - i + groups, groups)).wait_recv()
                if kind == "t":
                    pair_copy(i, j, p, parity).start()

    def landed(p):
        for part in range(PARTS[p]):
            y_landed(p, "g", part)
        if TREE_EIGHTHS[p]:
            for j in range(1, routers):
                for i in range(groups):
                    pair_copy(i, j, p, 1 - parity).wait_recv()

    tile_slots = 4
    tile = tile_slots * width
    tiles = rows // tile

    def x_tile(i):
        return x_all[pl.ds(i * tile_slots, tile_slots)].reshape(tile, model)

    def span_of(i):
        return pl.ds(pl.multiple_of(i * tile, tile), tile)

    def projected(p, i):
        x = x_tile(i)
        total = jnp.zeros((tile, half_width), F32)
        for a in range(routers):
            total = total + jnp.dot(
                x[:, a * depth : (a + 1) * depth], w_all[p, a], preferred_element_type=F32
            )
        return silu(total)

    def query(i):
        q_v[span_of(i), :] = projected(0, i).astype(BF16)

    def attend(i):
        span = span_of(i)
        for e in range(heads_here):
            cols = slice(e * HEAD_DIM, (e + 1) * HEAD_DIM)
            raw = lax.dot_general(
                q_v[span, cols],
                keys_v[:, :, cols].reshape(positions, HEAD_DIM),
                (((1,), (1,)), ((), ())),
                preferred_element_type=F32,
            )
            weights = silu(raw * scale)
            parts = []
            for s in range(tile_slots):
                line = mask_all[i * (tile_slots // CAP) + s // CAP, s % CAP : s % CAP + 1, :]
                parts.append(weights[s * width : (s + 1) * width] * line)
            weights = jnp.concatenate(parts, axis=0).astype(BF16)
            att_v[span, cols] = (
                jnp.dot(
                    weights,
                    values_v[:, :, cols].reshape(positions, HEAD_DIM),
                    preferred_element_type=F32,
                )
                .astype(BF16)
                .astype(F32)
            )

    def self_key(i):
        span = span_of(i)
        keys = projected(1, i)
        for e in range(heads_here):
            cols = slice(e * HEAD_DIM, (e + 1) * HEAD_DIM)
            own = jnp.sum(q_v[span, cols].astype(F32) * keys[:, cols], axis=1, keepdims=True)
            own_v[span, cols] = jnp.broadcast_to(silu(own * scale), (tile, HEAD_DIM))

    lane = lax.broadcasted_iota(jnp.int32, (tile, 128), 1)

    def self_value(i):
        span = span_of(i)
        att = att_v[span, :] + own_v[span, :] * projected(2, i)
        att_v[span, :] = att
        total = jnp.sum(att, axis=1, keepdims=True)
        square = jnp.sum(att * att, axis=1, keepdims=True)
        stat_out[span, :] = jnp.where(lane == 0, total, square)

    def gate(i):
        span = span_of(i)
        both = stat_out[span, :] + stat_in[span, :]
        mean = both[:, 0:1] / hd_all
        var = both[:, 1:2] / hd_all - mean * mean
        gated_v[span, :] = (
            (att_v[span, :] - mean)
            * lax.rsqrt(var + EPSILON)
            * attn_gain_ref[...].astype(F32).reshape(1, -1)
            * projected(3, i)
        ).astype(BF16)

    with jax.named_scope("fwd0"):
        for part in range(PARTS[0]):
            forward(0, "g", part)
    with jax.named_scope("fwd1"):
        forward(1, "t")
        forward(2, "t")
    with jax.named_scope("items"):
        for k in range(1, users):
            z_copy(k, lax.rem(me - k + users, users)).wait_recv()
            relay_copy(k, h).start()
    with jax.named_scope("fwd1b"):
        forward(1, "g")
        y_landed(1, "t")
    with jax.named_scope("items2"):
        for k in range(1, users):
            m_copy(k, lax.rem(me - k + users, users)).wait_recv()
            relay_copy(k, mate).wait_recv()
        c_win.wait()
    with jax.named_scope("land0"):
        landed(0)
    with jax.named_scope("query"):
        pl.loop(0, tiles)(query)
    with jax.named_scope("fwd3a"):
        forward(3, "t")
        y_landed(2, "t")
    c_keys.wait()
    c_values.wait()
    with jax.named_scope("attend0"):
        pl.loop(0, tiles // 2)(attend)
    with jax.named_scope("fwd4a"):
        forward(4, "t")
    with jax.named_scope("attend1"):
        pl.loop(tiles // 2, tiles)(attend)
    with jax.named_scope("fwd2b"):
        forward(2, "g")
    with jax.named_scope("land1"):
        landed(1)
    with jax.named_scope("key"):
        pl.loop(0, tiles)(self_key)
    with jax.named_scope("fwd3b"):
        forward(3, "g")
        y_landed(3, "t")
        forward(4, "g", 0)
        y_landed(4, "t")
        forward(4, "g", 1)
    with jax.named_scope("land2"):
        landed(2)
    with jax.named_scope("value0"):
        pl.loop(0, tiles // 2)(self_value)
    with jax.named_scope("fwd4c"):
        forward(4, "g", 2)
    with jax.named_scope("value1"):
        pl.loop(tiles // 2, tiles)(self_value)

    stat_copy = pltpu.make_async_remote_copy(
        src_ref=stat_out,
        dst_ref=stat_in,
        send_sem=st_sem.at[0],
        recv_sem=st_sem.at[1],
        device_id={"heads": mate},
        device_id_type=MESH,
    )
    stat_copy.start()
    with jax.named_scope("fwd4b"):
        forward(4, "g", 3)
    with jax.named_scope("land3"):
        landed(3)
    with jax.named_scope("statwait"):
        stat_copy.wait_recv()
    with jax.named_scope("gate"):
        pl.loop(0, tiles)(gate)

    half = rows // heads
    c_wo.wait()

    mine = users // heads
    piece = half // 2
    source_rows = CAP * width

    def far_first(e, i, amount):
        return jnp.where(me < e * mine + mine // 2, amount - 1 - i, i)

    def part_copy(j, c):
        spot = pl.ds(pl.multiple_of(c * piece, piece), piece)
        return pltpu.make_async_remote_copy(
            src_ref=part_out.at[j, spot, :],
            dst_ref=part_in.at[j, spot, :],
            send_sem=po_send.at[j, c],
            recv_sem=po_recv.at[j, c],
            device_id={"heads": mate},
            device_id_type=MESH,
        )

    def out_project(j, row_half, c, target):
        src = pl.ds(pl.multiple_of(row_half * half + c * piece, piece), piece)
        target[j, pl.ds(pl.multiple_of(c * piece, piece), piece), :] = jnp.dot(
            gated_v[src, :],
            wo_all[lax.rem(r - j + routers, routers)],
            preferred_element_type=F32,
        ).astype(target.dtype)

    def shares(j):
        for i in range(2):
            c = far_first(mate, i, 2)
            out_project(j, mate, c, part_out)
            part_copy(j, c).start()

    with jax.named_scope("outown"):
        shares(0)
        for c in range(2):
            out_project(0, h, c, part_own)
    with jax.named_scope("land4"):
        landed(4)
    for j in range(1, routers):
        shares(j)
    for j in range(1, routers):
        for c in range(2):
            out_project(j, h, c, part_own)
    c_one.wait()

    two = jnp.broadcast_to(
        w_two_ref[...].astype(F32).reshape(1, -1), (8, w_two_ref.shape[0])
    ).astype(BF16)

    def score(source, i):
        span = pl.ds(pl.multiple_of(source * source_rows, source_rows), source_rows)
        x = x_all[pl.ds((h * mine + source) * CAP, CAP)].reshape(source_rows, model).astype(F32)
        mixed = []
        for a in range(routers):
            j = lax.rem(r - a + routers, routers)
            mixed.append(part_own[j, span, :] + part_in[j, span, :].astype(F32))
        residual = x + jnp.concatenate(mixed, axis=1)
        norm = lax.rsqrt(jnp.sum(residual * residual, axis=1, keepdims=True) / model + EPSILON)
        normed = (residual * norm * mlp_gain_ref[...].astype(F32).reshape(1, -1)).astype(BF16)
        hidden = silu(jnp.dot(normed, w_one_v[...], preferred_element_type=F32)).astype(BF16)
        sc_out[i] = lax.dot_general(
            two, hidden, (((1,), (1,)), ((), ())), preferred_element_type=F32
        )

    def score_copy(i, e, owner, sem):
        return pltpu.make_async_remote_copy(
            src_ref=sc_out.at[i],
            dst_ref=ret.at[owner],
            send_sem=sc_send.at[i, e],
            recv_sem=sc_recv.at[sem],
            device_id={"users": h * mine + far_first(h, i, mine), "heads": e},
            device_id_type=MESH,
        )

    for i in range(mine):
        source = far_first(h, i, mine)
        if i % (mine // 2) == 0:
            with jax.named_scope("partwait"):
                for j in range(routers):
                    part_copy(j, far_first(h, i // (mine // 2), 2)).wait_recv()
        score(source, i)
        target = h * mine + source
        for e in range(heads):
            itself = (target == me) & (h == e)

            @pl.when(jnp.logical_not(itself))
            def _():
                score_copy(i, e, me, me).start()

            @pl.when(itself)
            def _():
                ret[me] = sc_out[i]

    handler = me // mine
    with jax.named_scope("scorewait"):
        for d in range(users):

            @pl.when(jnp.logical_not((d == me) & (h == handler)))
            def _():
                score_copy(0, 0, d, d).wait_recv()

    position = lax.broadcasted_iota(jnp.int32, (1, width), 1)
    for b in range(blocks):
        tile_in = ret[owners[b]]
        line = tile_in[0:1, 0:width]
        for cap in range(1, CAP):
            line = jnp.where(ranks[b] == cap, tile_in[0:1, cap * width : (cap + 1) * width], line)
        out_ref[b : b + 1, :] = jnp.where(position < fill_ref[b], line, 0.0)

    for t in range(len(pieces)):
        for j in range(1, routers):
            x_copy(j, t, r).wait_send()
            for i in range(1, groups):
                y_copy(i, j, t, g).wait_send()
    for p in range(5):
        if TREE_EIGHTHS[p]:
            for j in range(1, routers):
                for i in range(groups):
                    pair_copy(i, j, p, parity).wait_send()
    for k in range(1, users):
        z_copy(k, me).wait_send()
        m_copy(k, me).wait_send()
        relay_copy(k, h).wait_send()
    stat_copy.wait_send()
    for j in range(routers):
        for c in range(2):
            part_copy(j, c).wait_send()
    for i in range(mine):
        for e in range(heads):

            @pl.when(jnp.logical_not((h * mine + far_first(h, i, mine) == me) & (h == e)))
            def _():
                score_copy(i, e, me, me).wait_send()


def local(
    sizes,
    items,
    block_owner,
    block_user,
    block_fill,
    prefix_keys,
    prefix_values,
    w_in,
    attn_gain,
    w_o,
    mlp_gain,
    w_one,
    w_two,
):
    groups, users, routers, heads = sizes
    blocks, width, model = items.shape
    projections, depth, half_width = w_in.shape
    slots = users * CAP
    rows = slots * width
    half = rows // heads
    out_cols = w_o.shape[1]
    cached, per_user, _ = prefix_keys.shape
    positions = cached * per_user
    pieces = len(ORDER)
    dma = pltpu.SemaphoreType.DMA
    hbm = pl.BlockSpec(memory_space=pl.ANY)
    vmem = pl.BlockSpec(memory_space=pltpu.VMEM)
    smem = pl.BlockSpec(memory_space=pltpu.SMEM)
    scratch = [
        pltpu.VMEM((blocks, width, model), BF16),
        pltpu.VMEM((users, CAP, width // heads, model), BF16),
        pltpu.VMEM((slots, width, model), BF16),
        pltpu.VMEM((users, 8, positions), F32),
        pltpu.VMEM((users, 8, positions), F32),
        pltpu.VMEM(prefix_keys.shape, BF16),
        pltpu.VMEM(prefix_values.shape, BF16),
        pltpu.VMEM((projections, routers, depth, half_width), BF16),
        pltpu.VMEM((routers, half_width, out_cols), BF16),
        pltpu.VMEM(w_one.shape, BF16),
        pltpu.VMEM((rows, half_width), BF16),
        pltpu.VMEM((rows, half_width), F32),
        pltpu.VMEM((rows, half_width), F32),
        pltpu.VMEM((rows, half_width), BF16),
        pltpu.VMEM((rows, 128), F32),
        pltpu.VMEM((rows, 128), F32),
        pltpu.VMEM((routers, half, out_cols), BF16),
        pltpu.VMEM((routers, half, out_cols), F32),
        pltpu.VMEM((routers, half, out_cols), BF16),
        pltpu.VMEM((users // heads, 8, CAP * width), F32),
        pltpu.VMEM((users, 8, CAP * width), F32),
        dma((6,)),
        dma((users,)),
        dma((users,)),
        dma((users,)),
        dma((users,)),
        dma((users,)),
        dma((users,)),
        dma((routers, pieces)),
        dma((routers, pieces)),
        dma((groups, routers, pieces)),
        dma((groups, routers, pieces)),
        dma((groups, routers, 5)),
        dma((groups, routers, 5)),
        dma((2,)),
        dma((routers, 2)),
        dma((routers, 2)),
        dma((users // heads, heads)),
        dma((users,)),
    ]
    return pl.pallas_call(
        functools.partial(scorer, sizes),
        out_shape=jax.ShapeDtypeStruct((blocks, width), F32),
        in_specs=[hbm, smem, smem, smem, hbm, hbm, hbm, vmem, hbm, vmem, hbm, vmem],
        out_specs=vmem,
        scratch_shapes=scratch,
        compiler_params=pltpu.CompilerParams(
            collective_id=0, has_side_effects=True, vmem_limit_bytes=62 * 1024 * 1024
        ),
    )(
        items,
        block_owner.reshape(-1),
        block_user,
        block_fill,
        prefix_keys,
        prefix_values,
        w_in,
        attn_gain,
        w_o,
        mlp_gain,
        w_one,
        w_two,
    )


def solution(mesh):
    placed = (
        P(("groups", "users", "routers"), None, None),
        P(("groups", "users", "routers"), None),
        P(("groups", "users", "routers")),
        P(("groups", "users", "routers")),
        P(("groups", "users"), None, "heads"),
        P(("groups", "users"), None, "heads"),
        P(None, "routers", "heads"),
        P("heads"),
        P("heads", "routers"),
        P(),
        P(),
        P(),
    )
    sizes = tuple(mesh.shape[name] for name in ("groups", "users", "routers", "heads"))
    return jax.shard_map(
        functools.partial(local, sizes),
        mesh=mesh,
        in_specs=placed,
        out_specs=P(("groups", "users", "routers"), None),
        check_vma=False,
    )
```

```python
import functools
import math

import jax
import jax.numpy as jnp
from jax import lax
from jax.experimental import pallas as pl
from jax.experimental.pallas import tpu as pltpu
from jax.sharding import PartitionSpec as P

HEAD_DIM = 128
CAP = 2
EPSILON = 1e-05
TREE_EIGHTHS = (0, 5, 5, 5, 4)
PARTS = (4, 1, 1, 1, 4)
ORDER = (
    [(0, "g", part) for part in range(PARTS[0])]
    + [(1, "t", 0), (2, "t", 0), (1, "g", 0), (3, "t", 0), (4, "t", 0), (2, "g", 0), (3, "g", 0)]
    + [(4, "g", part) for part in range(PARTS[4])]
)
F32 = jnp.float32
BF16 = jnp.bfloat16
MESH = pl.DeviceIdType.MESH


def silu(v):
    return 0.5 * v * (1.0 + jnp.tanh(0.5 * v))


def scorer(
    sizes,
    items_ref,
    owner_ref,
    user_ref,
    fill_ref,
    keys_ref,
    values_ref,
    w_in_ref,
    attn_gain_ref,
    w_o_ref,
    mlp_gain_ref,
    w_one_ref,
    w_two_ref,
    out_ref,
    items_v,
    out_slots,
    x_all,
    mask_out,
    mask_all,
    keys_v,
    values_v,
    w_all,
    wo_all,
    w_one_v,
    q_v,
    own_v,
    att_v,
    gated_v,
    stat_out,
    stat_in,
    part_out,
    part_own,
    part_in,
    sc_out,
    ret,
    local_sem,
    z_send,
    z_recv,
    m_send,
    m_recv,
    rel_send,
    rel_recv,
    x_send,
    x_recv,
    y_send,
    y_recv,
    w_send,
    w_recv,
    st_sem,
    po_send,
    po_recv,
    sc_send,
    sc_recv,
):
    groups, users, routers, heads = sizes
    g = lax.axis_index("groups")
    me = lax.axis_index("users")
    r = lax.axis_index("routers")
    h = lax.axis_index("heads")
    mate = 1 - h
    blocks, width, model = items_v.shape
    slots = x_all.shape[0]
    half_width = q_v.shape[1]
    heads_here = half_width // HEAD_DIM
    hd_all = half_width * heads
    rows = slots * width
    depth = w_all.shape[2]
    out_cols = wo_all.shape[2]
    wh = width // heads
    scale = HEAD_DIM ** (-0.5)
    positions = keys_v.shape[0] * keys_v.shape[1]
    per_user = keys_v.shape[1]

    c_items = pltpu.make_async_copy(items_ref, items_v, local_sem.at[0])
    c_items.start()

    barrier = pltpu.get_barrier_semaphore()
    count = 0
    for j in range(1, routers):
        pl.semaphore_signal(
            barrier, inc=1, device_id={"routers": lax.rem(r + j, routers)}, device_id_type=MESH
        )
        count += 1
    for i in range(1, groups):
        pl.semaphore_signal(
            barrier, inc=1, device_id={"groups": lax.rem(g + i, groups)}, device_id_type=MESH
        )
        count += 1
    pl.semaphore_signal(barrier, inc=1, device_id={"heads": mate}, device_id_type=MESH)
    count += 1
    for k in range(1, users):
        for e in range(heads):
            pl.semaphore_signal(
                barrier,
                inc=1,
                device_id={"users": lax.rem(me + k, users), "heads": e},
                device_id_type=MESH,
            )
            count += 1
    c_keys = pltpu.make_async_copy(keys_ref, keys_v, local_sem.at[1])
    c_values = pltpu.make_async_copy(values_ref, values_v, local_sem.at[2])
    c_win = pltpu.make_async_copy(w_in_ref, w_all.at[:, r], local_sem.at[3])
    c_wo = pltpu.make_async_copy(w_o_ref, wo_all.at[r], local_sem.at[4])
    c_one = pltpu.make_async_copy(w_one_ref, w_one_v, local_sem.at[5])
    pl.semaphore_wait(barrier, count)

    pieces = ORDER
    number = {piece: t for t, piece in enumerate(pieces)}
    parity = lax.rem(me, 2)
    pair = me + 1 - 2 * parity

    def piece_rows(p, kind, part, owner_group, owner_parity):
        length = depth if p < 4 else half_width
        tree = length * TREE_EIGHTHS[p] // 8 // (2 * groups) // 16 * 16
        if kind == "t":
            return pl.ds(pl.multiple_of((owner_group * 2 + owner_parity) * tree, tree), tree)
        direct = length // groups - 2 * tree
        share = direct // PARTS[p]
        start = 2 * groups * tree + owner_group * direct + part * share
        return pl.ds(pl.multiple_of(start, math.gcd(share, 16)), share)

    def weight_slot(owner_router, owner_group, owner_parity, t):
        p, kind, part = pieces[t]
        span = piece_rows(p, kind, part, owner_group, owner_parity)
        if p < 4:
            return w_all.at[p, owner_router, span, :]
        return wo_all.at[owner_router, span, :]

    def x_copy(j, t, source_router):
        p, kind, part = pieces[t]
        span = piece_rows(p, kind, part, g, parity)
        src = w_in_ref.at[p, span, :] if p < 4 else w_o_ref.at[span, :]
        return pltpu.make_async_remote_copy(
            src_ref=src,
            dst_ref=weight_slot(source_router, g, parity, t),
            send_sem=x_send.at[j, t],
            recv_sem=x_recv.at[j, t],
            device_id={"routers": lax.rem(r + j, routers)},
            device_id_type=MESH,
        )

    def y_copy(i, j, t, owner_group):
        spot = weight_slot(lax.rem(r - j + routers, routers), owner_group, parity, t)
        return pltpu.make_async_remote_copy(
            src_ref=spot,
            dst_ref=spot,
            send_sem=y_send.at[i, j, t],
            recv_sem=y_recv.at[i, j, t],
            device_id={"groups": lax.rem(g + i, groups)},
            device_id_type=MESH,
        )

    def pair_copy(i, j, p, owner_parity):
        spot = weight_slot(
            lax.rem(r - j + routers, routers),
            lax.rem(g - i + groups, groups),
            owner_parity,
            number[p, "t", 0],
        )
        return pltpu.make_async_remote_copy(
            src_ref=spot,
            dst_ref=spot,
            send_sem=w_send.at[i, j, p],
            recv_sem=w_recv.at[i, j, p],
            device_id={"users": pair},
            device_id_type=MESH,
        )

    for t in range(len(pieces)):
        for j in range(1, routers):
            x_copy(j, t, r).start()
    for c in (c_win, c_keys, c_values, c_wo, c_one):
        c.start()

    owners = [owner_ref[b] for b in range(blocks)]
    ranks = []
    for b in range(blocks):
        rank = jnp.int32(0)
        for a in range(b):
            rank = rank + jnp.where(owners[a] == owners[b], 1, 0)
        ranks.append(rank)

    def slot_source(dest, cap):
        index, user = jnp.int32(0), jnp.int32(-1)
        for b in range(blocks):
            hit = (owners[b] == dest) & (ranks[b] == cap)
            index = jnp.where(hit, b, index)
            user = jnp.where(hit, user_ref[b], user)
        return index, user

    lane_user = lax.broadcasted_iota(jnp.int32, (1, positions), 1) // per_user
    mask_copies, item_copies = {}, {}

    def z_copy(k, source):
        return pltpu.make_async_remote_copy(
            src_ref=out_slots.at[k],
            dst_ref=x_all.at[pl.ds(source * CAP, CAP), pl.ds(pl.multiple_of(h * wh, wh), wh), :],
            send_sem=z_send.at[k],
            recv_sem=z_recv.at[k],
            device_id={"users": lax.rem(me + k, users)},
            device_id_type=MESH,
        )

    def m_copy(k, source):
        return pltpu.make_async_remote_copy(
            src_ref=mask_out.at[k],
            dst_ref=mask_all.at[source],
            send_sem=m_send.at[k],
            recv_sem=m_recv.at[k],
            device_id={"users": lax.rem(me + k, users)},
            device_id_type=MESH,
        )

    def relay_copy(k, part):
        source = lax.rem(me - k + users, users)
        spot = x_all.at[pl.ds(source * CAP, CAP), pl.ds(pl.multiple_of(part * wh, wh), wh), :]
        return pltpu.make_async_remote_copy(
            src_ref=spot,
            dst_ref=spot,
            send_sem=rel_send.at[k],
            recv_sem=rel_recv.at[k],
            device_id={"heads": mate},
            device_id_type=MESH,
        )

    c_items.wait()
    for k in list(range(1, users)) + [0]:
        dest = lax.rem(me + k, users)
        for cap in range(CAP):
            index, user = slot_source(dest, cap)
            line = jnp.where(lane_user == user, 1.0, 0.0).astype(F32)
            if k == 0:
                x_all[me * CAP + cap] = items_v[index]
                mask_all[me, cap : cap + 1, :] = line
            else:
                out_slots[k, cap] = items_v[index, pl.ds(pl.multiple_of(h * wh, wh), wh), :]
                mask_out[k, cap : cap + 1, :] = line
        if k:
            z_copy(k, me).start()
            m_copy(k, me).start()

    def forward(p, kind, part=0):
        t = number[p, kind, part]
        for j in range(1, routers):
            x_copy(j, t, lax.rem(r - j + routers, routers)).wait_recv()
            for i in range(1, groups):
                y_copy(i, j, t, g).start()
            if kind == "t":
                pair_copy(0, j, p, parity).start()

    def y_landed(p, kind, part=0):
        t = number[p, kind, part]
        for j in range(1, routers):
            for i in range(1, groups):
                y_copy(i, j, t, lax.rem(g - i + groups, groups)).wait_recv()
                if kind == "t":
                    pair_copy(i, j, p, parity).start()

    def landed(p):
        for part in range(PARTS[p]):
            y_landed(p, "g", part)
        if TREE_EIGHTHS[p]:
            for j in range(1, routers):
                for i in range(groups):
                    pair_copy(i, j, p, 1 - parity).wait_recv()

    tile_slots = 4
    tile = tile_slots * width
    tiles = rows // tile

    def x_tile(i):
        return x_all[pl.ds(i * tile_slots, tile_slots)].reshape(tile, model)

    def span_of(i):
        return pl.ds(pl.multiple_of(i * tile, tile), tile)

    def projected(p, i):
        x = x_tile(i)
        total = jnp.zeros((tile, half_width), F32)
        for a in range(routers):
            total = total + jnp.dot(
                x[:, a * depth : (a + 1) * depth], w_all[p, a], preferred_element_type=F32
            )
        return silu(total)

    def query(i):
        q_v[span_of(i), :] = projected(0, i).astype(BF16)

    def attend(i):
        span = span_of(i)
        for e in range(heads_here):
            cols = slice(e * HEAD_DIM, (e + 1) * HEAD_DIM)
            raw = lax.dot_general(
                q_v[span, cols],
                keys_v[:, :, cols].reshape(positions, HEAD_DIM),
                (((1,), (1,)), ((), ())),
                preferred_element_type=F32,
            )
            weights = silu(raw * scale)
            parts = []
            for s in range(tile_slots):
                line = mask_all[i * (tile_slots // CAP) + s // CAP, s % CAP : s % CAP + 1, :]
                parts.append(weights[s * width : (s + 1) * width] * line)
            weights = jnp.concatenate(parts, axis=0).astype(BF16)
            att_v[span, cols] = (
                jnp.dot(
                    weights,
                    values_v[:, :, cols].reshape(positions, HEAD_DIM),
                    preferred_element_type=F32,
                )
                .astype(BF16)
                .astype(F32)
            )

    def self_key(i):
        span = span_of(i)
        keys = projected(1, i)
        for e in range(heads_here):
            cols = slice(e * HEAD_DIM, (e + 1) * HEAD_DIM)
            own = jnp.sum(q_v[span, cols].astype(F32) * keys[:, cols], axis=1, keepdims=True)
            own_v[span, cols] = jnp.broadcast_to(silu(own * scale), (tile, HEAD_DIM))

    lane = lax.broadcasted_iota(jnp.int32, (tile, 128), 1)

    def self_value(i):
        span = span_of(i)
        att = att_v[span, :] + own_v[span, :] * projected(2, i)
        att_v[span, :] = att
        total = jnp.sum(att, axis=1, keepdims=True)
        square = jnp.sum(att * att, axis=1, keepdims=True)
        stat_out[span, :] = jnp.where(lane == 0, total, square)

    def gate(i):
        span = span_of(i)
        both = stat_out[span, :] + stat_in[span, :]
        mean = both[:, 0:1] / hd_all
        var = both[:, 1:2] / hd_all - mean * mean
        gated_v[span, :] = (
            (att_v[span, :] - mean)
            * lax.rsqrt(var + EPSILON)
            * attn_gain_ref[...].astype(F32).reshape(1, -1)
            * projected(3, i)
        ).astype(BF16)

    with jax.named_scope("fwd0"):
        for part in range(PARTS[0]):
            forward(0, "g", part)
    with jax.named_scope("fwd1"):
        forward(1, "t")
        forward(2, "t")
        forward(1, "g")
    with jax.named_scope("items"):
        for k in range(1, users):
            z_copy(k, lax.rem(me - k + users, users)).wait_recv()
            relay_copy(k, h).start()
    with jax.named_scope("fwd1b"):
        y_landed(1, "t")
    with jax.named_scope("items2"):
        for k in range(1, users):
            m_copy(k, lax.rem(me - k + users, users)).wait_recv()
            relay_copy(k, mate).wait_recv()
        c_win.wait()
    with jax.named_scope("land0"):
        landed(0)
    with jax.named_scope("query"):
        pl.loop(0, tiles)(query)
    with jax.named_scope("fwd3a"):
        forward(3, "t")
        y_landed(2, "t")
    c_keys.wait()
    c_values.wait()
    with jax.named_scope("attend0"):
        pl.loop(0, tiles // 2)(attend)
    with jax.named_scope("fwd4a"):
        forward(4, "t")
    with jax.named_scope("attend1"):
        pl.loop(tiles // 2, tiles)(attend)
    with jax.named_scope("fwd2b"):
        forward(2, "g")
    with jax.named_scope("land1"):
        landed(1)
    with jax.named_scope("key"):
        pl.loop(0, tiles)(self_key)
    with jax.named_scope("fwd3b"):
        forward(3, "g")
        y_landed(3, "t")
        forward(4, "g", 0)
        y_landed(4, "t")
        forward(4, "g", 1)
    with jax.named_scope("land2"):
        landed(2)
    with jax.named_scope("value0"):
        pl.loop(0, tiles // 2)(self_value)
    with jax.named_scope("fwd4c"):
        forward(4, "g", 2)
    with jax.named_scope("value1"):
        pl.loop(tiles // 2, tiles)(self_value)

    stat_copy = pltpu.make_async_remote_copy(
        src_ref=stat_out,
        dst_ref=stat_in,
        send_sem=st_sem.at[0],
        recv_sem=st_sem.at[1],
        device_id={"heads": mate},
        device_id_type=MESH,
    )
    stat_copy.start()
    with jax.named_scope("fwd4b"):
        forward(4, "g", 3)
    with jax.named_scope("land3"):
        landed(3)
    with jax.named_scope("statwait"):
        stat_copy.wait_recv()
    with jax.named_scope("gate"):
        pl.loop(0, tiles)(gate)

    half = rows // heads
    c_wo.wait()

    mine = users // heads
    piece = half // 2
    source_rows = CAP * width

    def far_first(e, i, amount):
        return jnp.where(me < e * mine + mine // 2, amount - 1 - i, i)

    def part_copy(j, c):
        spot = pl.ds(pl.multiple_of(c * piece, piece), piece)
        return pltpu.make_async_remote_copy(
            src_ref=part_out.at[j, spot, :],
            dst_ref=part_in.at[j, spot, :],
            send_sem=po_send.at[j, c],
            recv_sem=po_recv.at[j, c],
            device_id={"heads": mate},
            device_id_type=MESH,
        )

    def out_project(j, row_half, c, target):
        src = pl.ds(pl.multiple_of(row_half * half + c * piece, piece), piece)
        target[j, pl.ds(pl.multiple_of(c * piece, piece), piece), :] = jnp.dot(
            gated_v[src, :],
            wo_all[lax.rem(r - j + routers, routers)],
            preferred_element_type=F32,
        ).astype(target.dtype)

    def shares(j):
        for i in range(2):
            c = far_first(mate, i, 2)
            out_project(j, mate, c, part_out)
            part_copy(j, c).start()

    with jax.named_scope("outown"):
        shares(0)
        for c in range(2):
            out_project(0, h, c, part_own)
    with jax.named_scope("land4"):
        landed(4)
    for j in range(1, routers):
        shares(j)
    for j in range(1, routers):
        for c in range(2):
            out_project(j, h, c, part_own)
    c_one.wait()

    two = jnp.broadcast_to(
        w_two_ref[...].astype(F32).reshape(1, -1), (8, w_two_ref.shape[0])
    ).astype(BF16)

    def score(source, i):
        span = pl.ds(pl.multiple_of(source * source_rows, source_rows), source_rows)
        x = x_all[pl.ds((h * mine + source) * CAP, CAP)].reshape(source_rows, model).astype(F32)
        mixed = []
        for a in range(routers):
            j = lax.rem(r - a + routers, routers)
            mixed.append(part_own[j, span, :] + part_in[j, span, :].astype(F32))
        residual = x + jnp.concatenate(mixed, axis=1)
        norm = lax.rsqrt(jnp.sum(residual * residual, axis=1, keepdims=True) / model + EPSILON)
        normed = (residual * norm * mlp_gain_ref[...].astype(F32).reshape(1, -1)).astype(BF16)
        hidden = silu(jnp.dot(normed, w_one_v[...], preferred_element_type=F32)).astype(BF16)
        sc_out[i] = lax.dot_general(
            two, hidden, (((1,), (1,)), ((), ())), preferred_element_type=F32
        )

    def score_copy(i, e, owner, sem):
        return pltpu.make_async_remote_copy(
            src_ref=sc_out.at[i],
            dst_ref=ret.at[owner],
            send_sem=sc_send.at[i, e],
            recv_sem=sc_recv.at[sem],
            device_id={"users": h * mine + far_first(h, i, mine), "heads": e},
            device_id_type=MESH,
        )

    for i in range(mine):
        source = far_first(h, i, mine)
        if i % (mine // 2) == 0:
            with jax.named_scope("partwait"):
                for j in range(routers):
                    part_copy(j, far_first(h, i // (mine // 2), 2)).wait_recv()
        score(source, i)
        target = h * mine + source
        for e in range(heads):
            itself = (target == me) & (h == e)

            @pl.when(jnp.logical_not(itself))
            def _():
                score_copy(i, e, me, me).start()

            @pl.when(itself)
            def _():
                ret[me] = sc_out[i]

    handler = me // mine
    with jax.named_scope("scorewait"):
        for d in range(users):

            @pl.when(jnp.logical_not((d == me) & (h == handler)))
            def _():
                score_copy(0, 0, d, d).wait_recv()

    position = lax.broadcasted_iota(jnp.int32, (1, width), 1)
    for b in range(blocks):
        tile_in = ret[owners[b]]
        line = tile_in[0:1, 0:width]
        for cap in range(1, CAP):
            line = jnp.where(ranks[b] == cap, tile_in[0:1, cap * width : (cap + 1) * width], line)
        out_ref[b : b + 1, :] = jnp.where(position < fill_ref[b], line, 0.0)

    for t in range(len(pieces)):
        for j in range(1, routers):
            x_copy(j, t, r).wait_send()
            for i in range(1, groups):
                y_copy(i, j, t, g).wait_send()
    for p in range(5):
        if TREE_EIGHTHS[p]:
            for j in range(1, routers):
                for i in range(groups):
                    pair_copy(i, j, p, parity).wait_send()
    for k in range(1, users):
        z_copy(k, me).wait_send()
        m_copy(k, me).wait_send()
        relay_copy(k, h).wait_send()
    stat_copy.wait_send()
    for j in range(routers):
        for c in range(2):
            part_copy(j, c).wait_send()
    for i in range(mine):
        for e in range(heads):

            @pl.when(jnp.logical_not((h * mine + far_first(h, i, mine) == me) & (h == e)))
            def _():
                score_copy(i, e, me, me).wait_send()


def local(
    sizes,
    items,
    block_owner,
    block_user,
    block_fill,
    prefix_keys,
    prefix_values,
    w_in,
    attn_gain,
    w_o,
    mlp_gain,
    w_one,
    w_two,
):
    groups, users, routers, heads = sizes
    blocks, width, model = items.shape
    projections, depth, half_width = w_in.shape
    slots = users * CAP
    rows = slots * width
    half = rows // heads
    out_cols = w_o.shape[1]
    cached, per_user, _ = prefix_keys.shape
    positions = cached * per_user
    pieces = len(ORDER)
    dma = pltpu.SemaphoreType.DMA
    hbm = pl.BlockSpec(memory_space=pl.ANY)
    vmem = pl.BlockSpec(memory_space=pltpu.VMEM)
    smem = pl.BlockSpec(memory_space=pltpu.SMEM)
    scratch = [
        pltpu.VMEM((blocks, width, model), BF16),
        pltpu.VMEM((users, CAP, width // heads, model), BF16),
        pltpu.VMEM((slots, width, model), BF16),
        pltpu.VMEM((users, 8, positions), F32),
        pltpu.VMEM((users, 8, positions), F32),
        pltpu.VMEM(prefix_keys.shape, BF16),
        pltpu.VMEM(prefix_values.shape, BF16),
        pltpu.VMEM((projections, routers, depth, half_width), BF16),
        pltpu.VMEM((routers, half_width, out_cols), BF16),
        pltpu.VMEM(w_one.shape, BF16),
        pltpu.VMEM((rows, half_width), BF16),
        pltpu.VMEM((rows, half_width), F32),
        pltpu.VMEM((rows, half_width), F32),
        pltpu.VMEM((rows, half_width), BF16),
        pltpu.VMEM((rows, 128), F32),
        pltpu.VMEM((rows, 128), F32),
        pltpu.VMEM((routers, half, out_cols), BF16),
        pltpu.VMEM((routers, half, out_cols), F32),
        pltpu.VMEM((routers, half, out_cols), BF16),
        pltpu.VMEM((users // heads, 8, CAP * width), F32),
        pltpu.VMEM((users, 8, CAP * width), F32),
        dma((6,)),
        dma((users,)),
        dma((users,)),
        dma((users,)),
        dma((users,)),
        dma((users,)),
        dma((users,)),
        dma((routers, pieces)),
        dma((routers, pieces)),
        dma((groups, routers, pieces)),
        dma((groups, routers, pieces)),
        dma((groups, routers, 5)),
        dma((groups, routers, 5)),
        dma((2,)),
        dma((routers, 2)),
        dma((routers, 2)),
        dma((users // heads, heads)),
        dma((users,)),
    ]
    return pl.pallas_call(
        functools.partial(scorer, sizes),
        out_shape=jax.ShapeDtypeStruct((blocks, width), F32),
        in_specs=[hbm, smem, smem, smem, hbm, hbm, hbm, vmem, hbm, vmem, hbm, vmem],
        out_specs=vmem,
        scratch_shapes=scratch,
        compiler_params=pltpu.CompilerParams(
            collective_id=0, has_side_effects=True, vmem_limit_bytes=62 * 1024 * 1024
        ),
    )(
        items,
        block_owner.reshape(-1),
        block_user,
        block_fill,
        prefix_keys,
        prefix_values,
        w_in,
        attn_gain,
        w_o,
        mlp_gain,
        w_one,
        w_two,
    )


def solution(mesh):
    placed = (
        P(("groups", "users", "routers"), None, None),
        P(("groups", "users", "routers"), None),
        P(("groups", "users", "routers")),
        P(("groups", "users", "routers")),
        P(("groups", "users"), None, "heads"),
        P(("groups", "users"), None, "heads"),
        P(None, "routers", "heads"),
        P("heads"),
        P("heads", "routers"),
        P(),
        P(),
        P(),
    )
    sizes = tuple(mesh.shape[name] for name in ("groups", "users", "routers", "heads"))
    return jax.shard_map(
        functools.partial(local, sizes),
        mesh=mesh,
        in_specs=placed,
        out_specs=P(("groups", "users", "routers"), None),
        check_vma=False,
    )
```
